8 devices in a mesh: tg: 2 (over z, y), pp: 2 (over x), grp: 2 (over core).
Axes of the slice: x: 2, y: 2, z: 1, core: 2. Of those that a mesh axis runs over, the one named last changes fastest.
Arguments:
- hidden_in: bfloat16 [512, 1024], P(('pp', 'grp'))
- seq_lens: int32 [512], P(('pp', 'grp'))
- k_cache: bfloat16 [2, 512, 128, 16, 64], P(None, ('pp', 'grp'), None, 'tg')
- v_cache: bfloat16 [2, 512, 128, 16, 64], P(None, ('pp', 'grp'), None, 'tg')
- attn_gain: bfloat16 [2, 1024], P('pp')
- w_qkv: bfloat16 [2, 3072, 1024], P('pp', ('tg', 'grp'))
- w_o: bfloat16 [2, 1024, 1024], P('pp', None, ('tg', 'grp'))
- mlp_gain: bfloat16 [2, 1024], P('pp')
- w_gate_up: bfloat16 [2, 5632, 1024], P('pp', ('tg', 'grp'))
- w_down: bfloat16 [2, 1024, 2816], P('pp', None, ('tg', 'grp'))
Outputs:
- output 1: bfloat16 [512, 1024], P(('pp', 'grp'))
- output 2: bfloat16 [2, 512, 128, 16, 64], P(None, ('pp', 'grp'), None, 'tg')
- output 3: bfloat16 [2, 512, 128, 16, 64], P(None, ('pp', 'grp'), None, 'tg')
- output 4: bfloat16 [2, 3072, 1024], P(None, 'tg')
- output 5: bfloat16 [2, 5632, 1024], P(None, 'tg')
All inputs are finite; a program needn't handle non-finite values.
Results may differ from the reference program's by a relative error of at most 0.0160774.
Values are sent between devices in bfloat16 or wider.
A program may use at most 1 GiB of HBM per device.

```python
import jax
import jax.numpy as jnp
from jax import lax
import math

MODEL_DIM = 1024
FFN_DIM = 2816
HEADS = 16
KV_HEADS = 16
HEAD_DIM = 64
LAYERS = 2
GEN_TP = 2
TRAIN_TP = 4
BATCH = 512
CACHE_LEN = 128

ROPE_THETA = 500000.0
NORM_EPS = 1e-5
MASK_FILL = -1e30


def draw_lens(key):
    key_len, key_top = jax.random.split(key)
    drawn = jax.random.randint(key_len, (BATCH,), CACHE_LEN // 8, CACHE_LEN)
    top_row = jax.random.randint(key_top, (), 0, BATCH)
    return jnp.where(jnp.arange(BATCH) == top_row, CACHE_LEN - 1, drawn).astype(jnp.int32)


def setup_inputs(seed: int = 0) -> dict:
    key_list = jax.random.split(jax.random.key(seed), 11)
    qkv_rows = (HEADS + 2 * KV_HEADS) * HEAD_DIM
    cache_shape = (LAYERS, BATCH, CACHE_LEN, KV_HEADS, HEAD_DIM)
    key_scale = math.sqrt(0.5 * math.log(CACHE_LEN))
    hidden_in = jax.random.normal(key_list[0], (BATCH, MODEL_DIM), jnp.float32)
    seq_lens = draw_lens(key_list[1])
    k_cache = jax.random.normal(key_list[2], cache_shape, jnp.float32) * key_scale
    v_mean = jax.random.normal(key_list[3], (LAYERS, BATCH, 1, KV_HEADS, HEAD_DIM), jnp.float32)
    v_cache = 0.5 * v_mean + jax.random.normal(key_list[4], cache_shape, jnp.float32)
    attn_gain = jax.random.uniform(key_list[5], (LAYERS, MODEL_DIM), jnp.float32, 0.2, 1.8)
    w_qkv = jax.random.normal(key_list[6], (LAYERS, qkv_rows, MODEL_DIM), jnp.float32) * MODEL_DIM ** -0.5
    w_o = jax.random.normal(key_list[7], (LAYERS, MODEL_DIM, HEADS * HEAD_DIM), jnp.float32) * (HEADS * HEAD_DIM) ** -0.5
    mlp_gain = jax.random.uniform(key_list[8], (LAYERS, MODEL_DIM), jnp.float32, 0.5, 1.5)
    w_gate_up = jax.random.normal(key_list[9], (LAYERS, 2 * FFN_DIM, MODEL_DIM), jnp.float32) * MODEL_DIM ** -0.5
    w_down = jax.random.normal(key_list[10], (LAYERS, MODEL_DIM, FFN_DIM), jnp.float32) * FFN_DIM ** -0.5
    return {
        "hidden_in": hidden_in.astype(jnp.bfloat16),
        "seq_lens": seq_lens,
        "k_cache": k_cache.astype(jnp.bfloat16),
        "v_cache": v_cache.astype(jnp.bfloat16),
        "attn_gain": attn_gain.astype(jnp.bfloat16),
        "w_qkv": w_qkv.astype(jnp.bfloat16),
        "w_o": w_o.astype(jnp.bfloat16),
        "mlp_gain": mlp_gain.astype(jnp.bfloat16),
        "w_gate_up": w_gate_up.astype(jnp.bfloat16),
        "w_down": w_down.astype(jnp.bfloat16),
    }


def rms_norm(hidden, gain_vec):
    hidden_f32 = hidden.astype(jnp.float32)
    inv_rms = lax.rsqrt(jnp.mean(hidden_f32 * hidden_f32, axis=-1, keepdims=True) + NORM_EPS)
    return (hidden_f32 * inv_rms * gain_vec.astype(jnp.float32)).astype(jnp.bfloat16)


def apply_rope(values, cos_t, sin_t):
    half_dim = values.shape[-1] // 2
    first_half = values[..., :half_dim]
    second_half = values[..., half_dim:]
    return jnp.concatenate([first_half * cos_t - second_half * sin_t, second_half * cos_t + first_half * sin_t], axis=-1)


def reference(hidden_in, seq_lens, k_cache, v_cache, attn_gain, w_qkv, w_o, mlp_gain, w_gate_up, w_down):
    group_rep = HEADS // KV_HEADS
    blocks = w_qkv.reshape(LAYERS, KV_HEADS, group_rep + 2, HEAD_DIM, MODEL_DIM)
    w_query = blocks[:, :, :group_rep].reshape(LAYERS, HEADS * HEAD_DIM, MODEL_DIM)
    w_key = blocks[:, :, group_rep].reshape(LAYERS, KV_HEADS * HEAD_DIM, MODEL_DIM)
    w_value = blocks[:, :, group_rep + 1].reshape(LAYERS, KV_HEADS * HEAD_DIM, MODEL_DIM)
    gen_qkv = jnp.concatenate([
        w_query.reshape(LAYERS, GEN_TP, -1, MODEL_DIM),
        w_key.reshape(LAYERS, GEN_TP, -1, MODEL_DIM),
        w_value.reshape(LAYERS, GEN_TP, -1, MODEL_DIM)], axis=2).reshape(LAYERS, -1, MODEL_DIM)
    fused_rows = w_gate_up.reshape(LAYERS, TRAIN_TP, 2, FFN_DIM // TRAIN_TP, MODEL_DIM)
    w_gate = fused_rows[:, :, 0].reshape(LAYERS, FFN_DIM, MODEL_DIM)
    w_up = fused_rows[:, :, 1].reshape(LAYERS, FFN_DIM, MODEL_DIM)
    gen_gate_up = jnp.stack([
        w_gate.reshape(LAYERS, GEN_TP, -1, MODEL_DIM),
        w_up.reshape(LAYERS, GEN_TP, -1, MODEL_DIM)], axis=2).reshape(LAYERS, 2 * FFN_DIM, MODEL_DIM)

    positions = jnp.arange(CACHE_LEN)
    row_ids = jnp.arange(BATCH)
    inv_freq = jnp.power(ROPE_THETA, -jnp.arange(0, HEAD_DIM, 2).astype(jnp.float32) / HEAD_DIM)
    angles = seq_lens.astype(jnp.float32)[:, None] * inv_freq[None, :]
    cos_t = jnp.cos(angles)[:, None, :]
    sin_t = jnp.sin(angles)[:, None, :]
    score_scale = HEAD_DIM ** -0.5

    def attend_row(row_args):
        query_row, k_row, v_row, length = row_args
        query_grp = query_row.reshape(KV_HEADS, group_rep, HEAD_DIM).astype(jnp.float32)
        scores = jnp.einsum("grd,sgd->grs", query_grp, k_row.astype(jnp.float32)) * score_scale
        scores = jnp.where(positions[None, None, :] <= length, scores, MASK_FILL)
        attn_probs = jax.nn.softmax(scores, axis=-1).astype(jnp.bfloat16)
        out_row = jnp.einsum("grs,sgd->grd", attn_probs.astype(jnp.float32), v_row.astype(jnp.float32))
        return out_row.astype(jnp.bfloat16).reshape(HEADS * HEAD_DIM)

    def layer_step(hidden, layer_xs):
        gain_attn, wgt_query, wgt_key, wgt_value, wgt_out, gain_mlp, wgt_gate, wgt_up, wgt_down, k_layer, v_layer = layer_xs
        normed = rms_norm(hidden, gain_attn)
        query_vals = jnp.dot(normed, wgt_query.T, preferred_element_type=jnp.float32).reshape(BATCH, HEADS, HEAD_DIM)
        key_new = jnp.dot(normed, wgt_key.T, preferred_element_type=jnp.float32).reshape(BATCH, KV_HEADS, HEAD_DIM)
        value_new = jnp.dot(normed, wgt_value.T, preferred_element_type=jnp.float32).reshape(BATCH, KV_HEADS, HEAD_DIM).astype(jnp.bfloat16)
        query_vals = apply_rope(query_vals, cos_t, sin_t).astype(jnp.bfloat16)
        key_new = apply_rope(key_new, cos_t, sin_t).astype(jnp.bfloat16)
        k_layer = k_layer.at[row_ids, seq_lens].set(key_new)
        v_layer = v_layer.at[row_ids, seq_lens].set(value_new)
        attn_out = lax.map(attend_row, (query_vals, k_layer, v_layer, seq_lens))
        attn_proj = jnp.dot(attn_out, wgt_out.T, preferred_element_type=jnp.float32)
        hidden = (hidden.astype(jnp.float32) + attn_proj).astype(jnp.bfloat16)
        normed = rms_norm(hidden, gain_mlp)
        gate_vals = jnp.dot(normed, wgt_gate.T, preferred_element_type=jnp.float32)
        up_vals = jnp.dot(normed, wgt_up.T, preferred_element_type=jnp.float32)
        act_vals = (jax.nn.silu(gate_vals) * up_vals).astype(jnp.bfloat16)
        down_vals = jnp.dot(act_vals, wgt_down.T, preferred_element_type=jnp.float32)
        hidden = (hidden.astype(jnp.float32) + down_vals).astype(jnp.bfloat16)
        return hidden, (k_layer, v_layer)

    layer_xs = (attn_gain, w_query, w_key, w_value, w_o, mlp_gain, w_gate, w_up, w_down, k_cache, v_cache)
    hidden_out, cache_pair = lax.scan(layer_step, hidden_in, layer_xs)
    return (hidden_out, cache_pair[0], cache_pair[1], gen_qkv, gen_gate_up)
```

```python
import functools

import jax
import jax.numpy as jnp
from jax import lax
from jax.experimental import pallas as pl
from jax.experimental.pallas import tpu as pltpu
from jax.sharding import PartitionSpec as P

ROPE_THETA = 500000.0
NORM_EPS = 1e-5
MASK_FILL = -1e30
ROW_AXES = ("pp", "grp")
TRAIN_AXES = ("tg", "grp")
SWAP = ((0, 1), (1, 0))
F32 = jnp.float32
BF16 = jnp.bfloat16


def rms_norm(hidden, gain_vec):
    hidden_f32 = hidden.astype(F32)
    inv_rms = lax.rsqrt(jnp.mean(hidden_f32 * hidden_f32, axis=-1, keepdims=True) + NORM_EPS)
    return (hidden_f32 * inv_rms * gain_vec.astype(F32)).astype(BF16)


def rope_tables_t(seq_lens, head_dim):
    inv_freq = jnp.power(ROPE_THETA, -jnp.arange(0, head_dim, 2).astype(F32) / head_dim)
    angles = inv_freq[:, None] * seq_lens.astype(F32)[None, :]
    return jnp.cos(angles), jnp.sin(angles)


def place_kernel(idx_ref, piece_ref, *rest):
    rest[-1][...] = piece_ref[...].reshape(rest[-1].shape)


def place(piece, dst, dst_shape, in_block, in_map, out_block, out_map, steps, idx):
    in_specs = [pl.BlockSpec(in_block, in_map)]
    args = [piece]
    aliases = {}
    if dst is not None:
        in_specs.append(pl.BlockSpec(memory_space=pl.ANY))
        args.append(dst)
        aliases = {2: 0}
    return pl.pallas_call(
        place_kernel,
        grid_spec=pltpu.PrefetchScalarGridSpec(
            num_scalar_prefetch=1, grid=(steps,), in_specs=in_specs,
            out_specs=pl.BlockSpec(out_block, out_map)),
        out_shape=jax.ShapeDtypeStruct(dst_shape, piece.dtype),
        input_output_aliases=aliases,
        cost_estimate=pl.CostEstimate(flops=piece.size * 2000, bytes_accessed=piece.size * 4, transcendentals=0),
        name="place",
    )(idx, *args)


def attn_kernel(lens_ref, h_ref, gain_ref, w_ref, cos_ref, sin_ref, k_ref, v_ref, *rest,
                heads, head_dim, scale):
    o_ref, ko_ref, vo_ref, q_s, kt_s, vt_s, o_s = rest[-7:]
    rows = heads * head_dim
    batch = h_ref.shape[0]
    per = k_ref.shape[1]
    seq = k_ref.shape[-1]
    step = pl.program_id(0)

    @pl.when(step == 0)
    def _():
        normed = rms_norm(h_ref[...], gain_ref[...])
        half = head_dim // 2

        def proj(t):
            return lax.dot_general(w_ref[0, t * rows:(t + 1) * rows, :], normed, (((1,), (1,)), ((), ())),
                                   preferred_element_type=F32)

        def rope(vals):
            vals = vals.reshape(heads, 2, half, batch)
            lo, hi = vals[:, 0], vals[:, 1]
            cos_t, sin_t = cos_ref[...][None], sin_ref[...][None]
            out = jnp.stack([lo * cos_t - hi * sin_t, hi * cos_t + lo * sin_t], axis=1)
            return out.reshape(rows, batch)

        q_s[...] = rope(proj(0)).T.astype(BF16).astype(F32)
        kt_s[...] = rope(proj(1)).astype(BF16)
        vt_s[...] = proj(2).astype(BF16)

    def one(i, carry):
        b = step * per + i
        n = lens_ref[b]
        lane = lax.broadcasted_iota(jnp.int32, (batch, seq), 1)
        row = lax.broadcasted_iota(jnp.int32, (batch, seq), 0)
        pick = jnp.where((row == b) & (lane == n), 1.0, 0.0).astype(BF16)
        at_n = lax.broadcasted_iota(jnp.int32, (rows, seq), 1) == n
        k_new = jnp.dot(kt_s[...], pick, preferred_element_type=F32).astype(BF16)
        v_new = jnp.dot(vt_s[...], pick, preferred_element_type=F32).astype(BF16)
        k_all = jnp.where(at_n, k_new, k_ref[0, i].reshape(rows, seq))
        v_all = jnp.where(at_n, v_new, v_ref[0, i].reshape(rows, seq))
        ko_ref[0, i] = k_all.reshape(heads, head_dim, seq)
        vo_ref[0, i] = v_all.reshape(heads, head_dim, seq)
        head_of = lax.broadcasted_iota(jnp.int32, (heads, rows), 1) // head_dim
        mine = head_of == lax.broadcasted_iota(jnp.int32, (heads, rows), 0)
        q_diag = jnp.where(mine, q_s[pl.ds(b, 1), :], 0.0).astype(BF16)
        scores = jnp.dot(q_diag, k_all, preferred_element_type=F32) * scale
        seen = lax.broadcasted_iota(jnp.int32, (heads, seq), 1) <= n
        scores = jnp.where(seen, scores, MASK_FILL)
        top = jnp.max(scores, axis=-1, keepdims=True)
        expd = jnp.exp(scores - top)
        probs = (expd / jnp.sum(expd, axis=-1, keepdims=True)).astype(BF16)
        outs = lax.dot_general(probs, v_all, (((1,), (1,)), ((), ())), preferred_element_type=F32)
        o_s[pl.ds(i, 1), :] = jnp.sum(jnp.where(mine, outs, 0.0), axis=0, keepdims=True)
        return carry

    lax.fori_loop(0, per, one, 0, unroll=4)
    o_ref[...] = o_s[...].astype(BF16)


def attention(layer, hidden, gain, w_qkv, cos_t, sin_t, seq_lens, kc, vc, outs):
    layers, batch, heads, head_dim, seq = kc.shape
    rows = heads * head_dim
    model = hidden.shape[1]
    per = 16
    whole = lambda *shape: pl.BlockSpec(shape, lambda s, n: (0,) * len(shape))
    cache_block = pl.BlockSpec((1, per, heads, head_dim, seq), lambda s, n: (layer, s, 0, 0, 0))
    in_specs = [whole(batch, model), whole(1, model),
                pl.BlockSpec((1, 3 * rows, model), lambda s, n: (layer, 0, 0)),
                whole(head_dim // 2, batch), whole(head_dim // 2, batch), cache_block, cache_block]
    args = [seq_lens, hidden, gain, w_qkv, cos_t, sin_t, kc, vc]
    aliases = {}
    if outs is not None:
        in_specs += [pl.BlockSpec(memory_space=pl.ANY)] * 2
        args += list(outs)
        aliases = {8: 1, 9: 2}
    cache_shape = jax.ShapeDtypeStruct(kc.shape, kc.dtype)
    return pl.pallas_call(
        functools.partial(attn_kernel, heads=heads, head_dim=head_dim, scale=head_dim ** -0.5),
        grid_spec=pltpu.PrefetchScalarGridSpec(
            num_scalar_prefetch=1, grid=(batch // per,), in_specs=in_specs,
            out_specs=[pl.BlockSpec((per, rows), lambda s, n: (s, 0)), cache_block, cache_block],
            scratch_shapes=[pltpu.VMEM((batch, rows), F32), pltpu.VMEM((rows, batch), BF16),
                            pltpu.VMEM((rows, batch), BF16), pltpu.VMEM((per, rows), F32)]),
        out_shape=[jax.ShapeDtypeStruct((batch, rows), BF16), cache_shape, cache_shape],
        input_output_aliases=aliases,
        compiler_params=pltpu.CompilerParams(dimension_semantics=("arbitrary",), vmem_limit_bytes=48 << 20),
        cost_estimate=pl.CostEstimate(flops=40_000_000_000, bytes_accessed=kc.size * 4, transcendentals=0),
        name=f"attention_{layer}",
    )(*args)


def solution(mesh):
    cache_spec = P(None, ROW_AXES, None, "tg", None)
    in_specs = (P(ROW_AXES, None), P(ROW_AXES), cache_spec, cache_spec,
                P("pp", None), P("pp", TRAIN_AXES, None), P("pp", None, TRAIN_AXES),
                P("pp", None), P("pp", TRAIN_AXES, None), P("pp", None, TRAIN_AXES))
    out_specs = (P(ROW_AXES, None), cache_spec, cache_spec, P(None, "tg", None), P(None, "tg", None))

    def body(hidden_in, seq_lens, k_cache, v_cache, attn_gain, w_qkv, w_o, mlp_gain, w_gate_up, w_down):
        layers, batch, _, heads, head_dim = k_cache.shape
        model = hidden_in.shape[1]
        stage = lax.axis_index("pp")
        half = lax.axis_index("grp")
        groups = w_qkv.shape[1] // (3 * head_dim)
        ffn = w_gate_up.shape[1] // 2
        cols = w_o.shape[2]

        kc = jnp.transpose(k_cache, (0, 1, 3, 4, 2))
        vc = jnp.transpose(v_cache, (0, 1, 3, 4, 2))
        cos_t, sin_t = rope_tables_t(seq_lens, head_dim)

        swap = lambda x, axis: lax.ppermute(x, axis, SWAP)
        both = lambda x: (x, swap(x, "grp"))

        def four(x):
            across = swap(x, "pp")
            own = both(x)
            other = both(across)
            return list(zip(own + other, (
                (stage, half), (stage, 1 - half), (1 - stage, half), (1 - stage, 1 - half))))

        def fill(pieces, dst_shape, in_block, in_map, out_block, out_map, steps):
            dst = None
            for piece, (lay, sh) in pieces:
                idx = jnp.stack([lay, sh]).astype(jnp.int32)
                dst = place(piece, dst, dst_shape, in_block, in_map, out_block, out_map, steps, idx)
            return dst

        gains = jnp.stack([attn_gain[0], mlp_gain[0]])
        other_gains = swap(gains, "pp")
        first = jnp.where(stage == 0, gains, other_gains)
        second = jnp.where(stage == 0, other_gains, gains)

        gen_qkv = fill(four(w_qkv.reshape(groups, 3, head_dim, model)),
                       (layers, 3, 2, groups, head_dim, model),
                       (groups, 1, head_dim, model), lambda s, i, *_: (0, s, 0, 0),
                       (1, 1, 1, groups, head_dim, model), lambda s, i, *_: (i[0], s, i[1], 0, 0, 0), 3)
        gen_qkv = gen_qkv.reshape(layers, 6 * groups * head_dim, model)
        gen_o = fill(four(w_o[0]), (layers, model, 2 * cols), (model, cols), lambda s, i, *_: (0, 0),
                     (1, model, cols), lambda s, i, *_: (i[0], 0, i[1]), 1)
        gen_gu = fill(four(w_gate_up.reshape(2, ffn, model)), (layers, 2, 2, ffn, model),
                      (1, ffn, model), lambda s, i, *_: (s, 0, 0),
                      (1, 1, 1, ffn, model), lambda s, i, *_: (i[0], s, i[1], 0, 0), 2)
        gen_gu = gen_gu.reshape(layers, 4 * ffn, model)
        gen_down = fill(four(jnp.transpose(w_down[0])), (layers, 2, ffn, model), (ffn, model), lambda s, i, *_: (0, 0),
                        (1, 1, ffn, model), lambda s, i, *_: (i[0], i[1], 0, 0), 1)
        gen_down = gen_down.reshape(layers, 2 * ffn, model)

        hidden = hidden_in
        caches = None
        for layer, gain in enumerate((first, second)):
            o_vals, *caches = attention(layer, hidden, gain[0][None], gen_qkv, cos_t, sin_t,
                                        seq_lens, kc, vc, caches)
            part = jnp.einsum("bk,dk->bd", o_vals, gen_o[layer], preferred_element_type=F32)
            hidden = (hidden.astype(F32) + (part + swap(part, "tg"))).astype(BF16)
            normed = rms_norm(hidden, gain[1])
            gate_up = jnp.einsum("bd,rd->br", normed, gen_gu[layer], preferred_element_type=F32)
            act = (jax.nn.silu(gate_up[:, :2 * ffn]) * gate_up[:, 2 * ffn:]).astype(BF16)
            part = jnp.einsum("bf,fd->bd", act, gen_down[layer], preferred_element_type=F32)
            hidden = (hidden.astype(F32) + (part + swap(part, "tg"))).astype(BF16)

        restore = lambda x: jnp.transpose(x, (0, 1, 4, 2, 3))
        return hidden, restore(caches[0]), restore(caches[1]), gen_qkv, gen_gu

    return jax.shard_map(body, mesh=mesh, in_specs=in_specs, out_specs=out_specs, check_vma=False)
```

```python
import functools

import jax
import jax.numpy as jnp
from jax import lax
from jax.experimental import pallas as pl
from jax.experimental.pallas import tpu as pltpu
from jax.sharding import PartitionSpec as P

ROPE_THETA = 500000.0
NORM_EPS = 1e-5
MASK_FILL = -1e30
UNROLL = 16
ROW_AXES = ("pp", "grp")
TRAIN_AXES = ("tg", "grp")
SWAP = ((0, 1), (1, 0))
F32 = jnp.float32
BF16 = jnp.bfloat16


def rms_norm(hidden, gain_vec):
    hidden_f32 = hidden.astype(F32)
    inv_rms = lax.rsqrt(jnp.mean(hidden_f32 * hidden_f32, axis=-1, keepdims=True) + NORM_EPS)
    return (hidden_f32 * inv_rms * gain_vec.astype(F32)).astype(BF16)


def rope_tables_t(seq_lens, head_dim):
    inv_freq = jnp.power(ROPE_THETA, -jnp.arange(0, head_dim, 2).astype(F32) / head_dim)
    angles = inv_freq[:, None] * seq_lens.astype(F32)[None, :]
    return jnp.cos(angles), jnp.sin(angles)


def place_kernel(idx_ref, piece_ref, *rest):
    rest[-1][...] = piece_ref[...].reshape(rest[-1].shape)


def place(piece, dst, dst_shape, in_block, in_map, out_block, out_map, steps, idx):
    in_specs = [pl.BlockSpec(in_block, in_map)]
    args = [piece]
    aliases = {}
    if dst is not None:
        in_specs.append(pl.BlockSpec(memory_space=pl.ANY))
        args.append(dst)
        aliases = {2: 0}
    return pl.pallas_call(
        place_kernel,
        grid_spec=pltpu.PrefetchScalarGridSpec(
            num_scalar_prefetch=1, grid=(steps,), in_specs=in_specs,
            out_specs=pl.BlockSpec(out_block, out_map)),
        out_shape=jax.ShapeDtypeStruct(dst_shape, piece.dtype),
        input_output_aliases=aliases,
        cost_estimate=pl.CostEstimate(flops=piece.size * 2000, bytes_accessed=piece.size * 4, transcendentals=0),
        name="place",
    )(idx, *args)


def attn_kernel(lens_ref, h_ref, gain_ref, w_ref, cos_ref, sin_ref, k_ref, v_ref, *rest,
                heads, head_dim, scale, row0):
    o_ref, ko_ref, vo_ref, q_s, kt_s, vt_s, o_s, p_s = rest[-8:]
    rows = heads * head_dim
    per = k_ref.shape[1]
    seq = k_ref.shape[-1]
    batch = seq
    step = pl.program_id(0)

    @pl.when(step == 0)
    def _():
        normed = rms_norm(h_ref[...], gain_ref[...])
        normed = jnp.concatenate([normed] * (batch // h_ref.shape[0]), axis=0)
        half = head_dim // 2

        def proj(t):
            return lax.dot_general(w_ref[0, t * rows:(t + 1) * rows, :], normed, (((1,), (1,)), ((), ())),
                                   preferred_element_type=F32)

        def rope(vals):
            vals = vals.reshape(heads, 2, half, batch)
            lo, hi = vals[:, 0], vals[:, 1]
            cos_t, sin_t = cos_ref[...][None], sin_ref[...][None]
            out = jnp.stack([lo * cos_t - hi * sin_t, hi * cos_t + lo * sin_t], axis=1)
            return out.reshape(rows, batch)

        q_s[...] = rope(proj(0)).T.astype(BF16).astype(F32)
        kt_s[...] = rope(proj(1))
        vt_s[...] = proj(2)

    lane = lax.broadcasted_iota(jnp.int32, (1, seq), 1)
    head_of = lax.broadcasted_iota(jnp.int32, (heads, rows), 1) // head_dim
    mine = head_of == lax.broadcasted_iota(jnp.int32, (heads, rows), 0)

    def insert(i, carry):
        b = step * per + i
        n = lens_ref[row0 + b]
        shift = lax.rem(n - b + seq, seq)
        at_n = jnp.broadcast_to(lane == n, (rows, seq))
        k_new = pltpu.roll(kt_s[...], shift, 1).astype(BF16)
        v_new = pltpu.roll(vt_s[...], shift, 1).astype(BF16)
        k_all = jnp.where(at_n, k_new, k_ref[0, i].reshape(rows, seq))
        v_all = jnp.where(at_n, v_new, v_ref[0, i].reshape(rows, seq))
        ko_ref[0, i] = k_all.reshape(heads, head_dim, seq)
        vo_ref[0, i] = v_all.reshape(heads, head_dim, seq)
        q_diag = jnp.where(mine, q_s[pl.ds(b, 1), :], 0.0).astype(BF16)
        scores = jnp.dot(q_diag, k_all, preferred_element_type=F32) * scale
        p_s[pl.ds(pl.multiple_of(i * heads, heads), heads), :] = jnp.where(lane <= n, scores, MASK_FILL)
        return carry

    lax.fori_loop(0, per, insert, 0, unroll=UNROLL)
    scores = p_s[...]
    expd = jnp.exp(scores - jnp.max(scores, axis=-1, keepdims=True))
    p_s[...] = (expd / jnp.sum(expd, axis=-1, keepdims=True)).astype(BF16).astype(F32)

    def combine(i, carry):
        probs = p_s[pl.ds(pl.multiple_of(i * heads, heads), heads), :].astype(BF16)
        outs = lax.dot_general(probs, vo_ref[0, i].reshape(rows, seq), (((1,), (1,)), ((), ())),
                               preferred_element_type=F32)
        o_s[pl.ds(i, 1), :] = jnp.sum(jnp.where(mine, outs, 0.0), axis=0, keepdims=True)
        return carry

    lax.fori_loop(0, per, combine, 0, unroll=UNROLL)
    o_ref[...] = o_s[...].astype(BF16)


def attention(layer, part, parts, hidden, gain, w_qkv, cos_t, sin_t, seq_lens, kc, vc, outs):
    layers, batch, heads, head_dim, seq = kc.shape
    rows = heads * head_dim
    count, model = hidden.shape
    per = 16
    first = part * count // per
    whole = lambda *shape: pl.BlockSpec(shape, lambda s, n: (0,) * len(shape))
    cache_block = pl.BlockSpec((1, per, heads, head_dim, seq), lambda s, n: (layer, first + s, 0, 0, 0))
    in_specs = [whole(count, model), whole(1, model),
                pl.BlockSpec((1, 3 * rows, model), lambda s, n: (layer, 0, 0)),
                whole(head_dim // 2, seq), whole(head_dim // 2, seq), cache_block, cache_block]
    args = [seq_lens, hidden, gain, w_qkv, cos_t, sin_t, kc, vc]
    aliases = {}
    if outs is not None:
        in_specs += [pl.BlockSpec(memory_space=pl.ANY)] * 2
        args += list(outs)
        aliases = {8: 1, 9: 2}
    cache_shape = jax.ShapeDtypeStruct(kc.shape, kc.dtype)
    return pl.pallas_call(
        functools.partial(attn_kernel, heads=heads, head_dim=head_dim, scale=head_dim ** -0.5, row0=part * count),
        grid_spec=pltpu.PrefetchScalarGridSpec(
            num_scalar_prefetch=1, grid=(count // per,), in_specs=in_specs,
            out_specs=[pl.BlockSpec((per, rows), lambda s, n: (s, 0)), cache_block, cache_block],
            scratch_shapes=[pltpu.VMEM((seq, rows), F32), pltpu.VMEM((rows, seq), F32),
                            pltpu.VMEM((rows, seq), F32), pltpu.VMEM((per, rows), F32),
                            pltpu.VMEM((per * heads, seq), F32)]),
        out_shape=[jax.ShapeDtypeStruct((count, rows), BF16), cache_shape, cache_shape],
        input_output_aliases=aliases,
        compiler_params=pltpu.CompilerParams(dimension_semantics=("arbitrary",), vmem_limit_bytes=48 << 20),
        cost_estimate=pl.CostEstimate(flops=30_000_000_000 // parts, bytes_accessed=kc.size * 4 // parts,
                                      transcendentals=0),
        name=f"attention_{layer}_{part}",
    )(*args)


def solution(mesh):
    cache_spec = P(None, ROW_AXES, None, "tg", None)
    in_specs = (P(ROW_AXES, None), P(ROW_AXES), cache_spec, cache_spec,
                P("pp", None), P("pp", TRAIN_AXES, None), P("pp", None, TRAIN_AXES),
                P("pp", None), P("pp", TRAIN_AXES, None), P("pp", None, TRAIN_AXES))
    out_specs = (P(ROW_AXES, None), cache_spec, cache_spec, P(None, "tg", None), P(None, "tg", None))

    def body(hidden_in, seq_lens, k_cache, v_cache, attn_gain, w_qkv, w_o, mlp_gain, w_gate_up, w_down):
        layers, batch, _, heads, head_dim = k_cache.shape
        model = hidden_in.shape[1]
        stage = lax.axis_index("pp")
        rank = lax.axis_index("tg")
        half = lax.axis_index("grp")
        groups = w_qkv.shape[1] // (3 * head_dim)
        ffn = w_gate_up.shape[1] // 2
        cols = w_o.shape[2]
        swap = lambda x, axis: lax.ppermute(x, axis, SWAP)

        def after(x, *deps):
            return lax.optimization_barrier((x,) + deps)[0]

        kc = jnp.transpose(k_cache, (0, 1, 3, 4, 2))
        vc = jnp.transpose(v_cache, (0, 1, 3, 4, 2))

        shard_qkv = w_qkv.reshape(groups, 3, head_dim, model)
        far_qkv = swap(shard_qkv, "pp")
        gains = jnp.stack([attn_gain[0], mlp_gain[0]])
        far_gains = swap(gains, "pp")
        near_qkv = swap(shard_qkv, "grp")
        shard_o = w_o[0]
        near_o = swap(shard_o, "grp")
        shard_down = jnp.transpose(w_down[0])
        near_gu = swap(w_gate_up[0], "grp")
        near_down = swap(shard_down, "grp")
        far_o = swap(after(shard_o, far_qkv), "pp")
        far_near_qkv = swap(far_qkv, "grp")
        far_near_o = swap(far_o, "grp")

        def ordered(own, near):
            return jnp.concatenate([jnp.where(half == 0, own, near), jnp.where(half == 0, near, own)], axis=1)

        stage_o, away_o = ordered(shard_o, near_o), ordered(far_o, far_near_o)
        rank_o = (jnp.where(stage == 0, stage_o, away_o), jnp.where(stage == 0, away_o, stage_o))
        peer_o = tuple(swap(w, "tg") for w in rank_o)

        cos_t, sin_t = rope_tables_t(seq_lens, head_dim)

        spots = ((stage, half), (stage, 1 - half), (1 - stage, half), (1 - stage, 1 - half))
        spots = [jnp.stack(spot).astype(jnp.int32) for spot in spots]

        qkv_place = functools.partial(
            place, dst_shape=(layers, 3, 2, groups, head_dim, model),
            in_block=(groups, 1, head_dim, model), in_map=lambda s, i, *_: (0, s, 0, 0),
            out_block=(1, 1, 1, groups, head_dim, model), out_map=lambda s, i, *_: (i[0], s, i[1], 0, 0, 0), steps=3)
        gen_qkv = None
        for piece, idx in zip((shard_qkv, near_qkv, far_qkv, far_near_qkv), spots):
            gen_qkv = qkv_place(piece, gen_qkv, idx=idx)
        gen_qkv = gen_qkv.reshape(layers, 6 * groups * head_dim, model)

        gu_shape = (layers, 2, 2, ffn, model)
        gu_place = functools.partial(
            place, dst_shape=gu_shape, in_block=(1, ffn, model), in_map=lambda s, i, *_: (s, 0, 0),
            out_block=(1, 1, 1, ffn, model), out_map=lambda s, i, *_: (i[0], s, i[1], 0, 0), steps=2)
        gen_gu = gu_place(w_gate_up.reshape(2, ffn, model), None, idx=spots[0])
        gen_gu = gu_place(near_gu.reshape(2, ffn, model), gen_gu, idx=spots[1])

        chunk = ffn // 2

        def gu_send(c, *deps):
            return swap(after(w_gate_up[0, c * chunk:(c + 1) * chunk], *deps), "pp")

        def gu_take(c, piece, dst):
            put = functools.partial(
                place, dst_shape=gu_shape, in_block=(chunk, model), in_map=lambda s, i, *_: (0, 0),
                out_block=(1, 1, 1, chunk, model), out_map=lambda s, i, *_: (i[0], c // 2, i[1], c % 2, 0), steps=1)
            dst = put(piece, dst, idx=spots[2])
            return put(swap(piece, "grp"), dst, idx=spots[3])

        def mlp(rows_in, gain):
            normed = rms_norm(rows_in, gain)
            total = 0.0
            for gu, down in ((w_gate_up[0], shard_down), (near_gu, near_down)):
                gate_up = jnp.einsum("bd,rd->br", normed, gu, preferred_element_type=F32)
                act = (jax.nn.silu(gate_up[:, :ffn]) * gate_up[:, ffn:]).astype(BF16)
                total = total + jnp.einsum("bf,fd->bd", act, down, preferred_element_type=F32)
            return total

        first = jnp.where(stage == 0, gains, far_gains)
        second = jnp.where(stage == 0, far_gains, gains)
        sent = [gu_send(0, far_o), gu_send(1, far_o)]
        hidden = hidden_in
        caches = None
        mid = batch // 2
        mine_rows = lambda x: lax.dynamic_slice_in_dim(x, rank * mid, mid, 0)
        peer_rows = lambda x: lax.dynamic_slice_in_dim(x, (1 - rank) * mid, mid, 0)
        for layer, gain in enumerate((first, second)):
            o_vals, *caches = attention(layer, 0, 1, hidden, gain[0][None], gen_qkv, cos_t, sin_t,
                                        seq_lens, kc, vc, caches)
            if layer == 1:
                o_vals = after(o_vals, sent[3])
            o_peer = swap(o_vals, "tg")
            proj = (jnp.einsum("bk,dk->bd", o_vals, rank_o[layer], preferred_element_type=F32)
                    + jnp.einsum("bk,dk->bd", o_peer, peer_o[layer], preferred_element_type=F32))
            hidden = (hidden.astype(F32) + proj).astype(BF16)
            if layer == 0:
                hidden = after(hidden, *sent)
            away = swap(hidden, "pp")
            if layer == 0:
                sent.append(gu_send(2, away))
            part = mlp(jnp.concatenate([hidden, away], axis=0), mlp_gain[0])
            keep = jnp.concatenate([mine_rows(part[:batch]), mine_rows(part[batch:])], axis=0)
            give = jnp.concatenate([peer_rows(part[:batch]), peer_rows(part[batch:])], axis=0)
            base = jnp.concatenate([mine_rows(hidden), mine_rows(away)], axis=0).astype(F32)
            done = (base + (keep + swap(give, "tg"))).astype(BF16)
            if layer == 0:
                done = after(done, sent[2])
            back = swap(done[mid:], "pp")
            if layer == 0:
                sent.append(gu_send(3, back))
            block = jnp.where(stage == layer, done[:mid], back)
            other = swap(block, "tg")
            hidden = jnp.concatenate([jnp.where(rank == 0, block, other), jnp.where(rank == 0, other, block)], axis=0)
        for c, piece in enumerate(sent):
            gen_gu = gu_take(c, piece, gen_gu)

        restore = lambda x: jnp.transpose(x, (0, 1, 4, 2, 3))
        return (hidden, restore(caches[0]), restore(caches[1]), gen_qkv, gen_gu.reshape(layers, 4 * ffn, model))

    return jax.shard_map(body, mesh=mesh, in_specs=in_specs, out_specs=out_specs, check_vma=False)
```

```python
import functools

import jax
import jax.numpy as jnp
from jax import lax
from jax.experimental import pallas as pl
from jax.experimental.pallas import tpu as pltpu
from jax.sharding import PartitionSpec as P

ROPE_THETA = 500000.0
NORM_EPS = 1e-5
MASK_FILL = -1e30
UNROLL = 16
PARTS = 2
ROW_AXES = ("pp", "grp")
TRAIN_AXES = ("tg", "grp")
SWAP = ((0, 1), (1, 0))
F32 = jnp.float32
BF16 = jnp.bfloat16


def rms_norm(hidden, gain_vec):
    hidden_f32 = hidden.astype(F32)
    inv_rms = lax.rsqrt(jnp.mean(hidden_f32 * hidden_f32, axis=-1, keepdims=True) + NORM_EPS)
    return (hidden_f32 * inv_rms * gain_vec.astype(F32)).astype(BF16)


def rope_tables_t(seq_lens, head_dim):
    inv_freq = jnp.power(ROPE_THETA, -jnp.arange(0, head_dim, 2).astype(F32) / head_dim)
    angles = inv_freq[:, None] * seq_lens.astype(F32)[None, :]
    return jnp.cos(angles), jnp.sin(angles)


def place_kernel(spots_ref, *refs, count, parts, targets, alias):
    pieces = refs[:count]
    dst = refs[count + alias]
    bufs = refs[count + alias + 1:2 * count + alias + 1]
    sem_in, sem_out = refs[-2:]
    reads, writes = [], []
    for i in range(count):
        for t in range(parts):
            reads.append(pltpu.make_async_copy(pieces[i].at[t], bufs[i].at[t], sem_in.at[i * parts + t]))
            reads[-1].start()
    for i in range(count):
        for t in range(parts):
            reads[i * parts + t].wait()
            spot = targets(spots_ref[i, 0], spots_ref[i, 1], t)
            writes.append(pltpu.make_async_copy(bufs[i].at[t], dst.at[spot], sem_out.at[i * parts + t]))
            writes[-1].start()
    for write in writes:
        write.wait()


def place(pieces, spots, dst, dst_shape, targets):
    count, parts = len(pieces), pieces[0].shape[0]
    alias = int(dst is not None)
    size = sum(p.size for p in pieces)
    return pl.pallas_call(
        functools.partial(place_kernel, count=count, parts=parts, targets=targets, alias=alias),
        in_specs=[pl.BlockSpec(memory_space=pltpu.SMEM)] + [pl.BlockSpec(memory_space=pl.ANY)] * (count + alias),
        out_specs=pl.BlockSpec(memory_space=pl.ANY),
        out_shape=jax.ShapeDtypeStruct(dst_shape, BF16),
        scratch_shapes=[pltpu.VMEM(p.shape, BF16) for p in pieces] + [
            pltpu.SemaphoreType.DMA((count * parts,)), pltpu.SemaphoreType.DMA((count * parts,))],
        input_output_aliases={count + 1: 0} if alias else {},
        compiler_params=pltpu.CompilerParams(vmem_limit_bytes=(2 * size + (2 << 20))),
        cost_estimate=pl.CostEstimate(flops=size * 3000, bytes_accessed=size * 4, transcendentals=0),
        name="place",
    )(jnp.stack(spots), *pieces, *([dst] if alias else []))


def attn_kernel(lens_ref, h_ref, gain_ref, w_ref, cos_ref, sin_ref, k_ref, v_ref, *rest,
                heads, head_dim, scale, row0):
    o_ref, ko_ref, vo_ref, q_s, kt_s, vt_s, o_s, p_s = rest[-8:]
    rows = heads * head_dim
    per = k_ref.shape[1]
    seq = k_ref.shape[-1]
    batch = seq
    step = pl.program_id(0)

    @pl.when(step == 0)
    def _():
        normed = rms_norm(h_ref[...], gain_ref[...])
        normed = jnp.concatenate([normed] * (batch // h_ref.shape[0]), axis=0)
        half = head_dim // 2

        def proj(t):
            return lax.dot_general(w_ref[0, t * rows:(t + 1) * rows, :], normed, (((1,), (1,)), ((), ())),
                                   preferred_element_type=F32)

        def rope(vals):
            vals = vals.reshape(heads, 2, half, batch)
            lo, hi = vals[:, 0], vals[:, 1]
            cos_t, sin_t = cos_ref[...][None], sin_ref[...][None]
            out = jnp.stack([lo * cos_t - hi * sin_t, hi * cos_t + lo * sin_t], axis=1)
            return out.reshape(rows, batch)

        q_s[...] = rope(proj(0)).T.astype(BF16).astype(F32)
        kt_s[...] = rope(proj(1))
        vt_s[...] = proj(2)

    lane = lax.broadcasted_iota(jnp.int32, (1, seq), 1)
    head_of = lax.broadcasted_iota(jnp.int32, (heads, rows), 1) // head_dim
    mine = head_of == lax.broadcasted_iota(jnp.int32, (heads, rows), 0)

    def insert(i, carry):
        b = row0 + step * per + i
        n = lens_ref[b]
        shift = lax.rem(n - b + seq, seq)
        at_n = jnp.broadcast_to(lane == n, (rows, seq))
        k_new = pltpu.roll(kt_s[...], shift, 1).astype(BF16)
        v_new = pltpu.roll(vt_s[...], shift, 1).astype(BF16)
        k_all = jnp.where(at_n, k_new, k_ref[0, i].reshape(rows, seq))
        v_all = jnp.where(at_n, v_new, v_ref[0, i].reshape(rows, seq))
        ko_ref[0, i] = k_all.reshape(heads, head_dim, seq)
        vo_ref[0, i] = v_all.reshape(heads, head_dim, seq)
        q_diag = jnp.where(mine, q_s[pl.ds(b, 1), :], 0.0).astype(BF16)
        scores = jnp.dot(q_diag, k_all, preferred_element_type=F32) * scale
        p_s[pl.ds(pl.multiple_of(i * heads, heads), heads), :] = jnp.where(lane <= n, scores, MASK_FILL)
        return carry

    lax.fori_loop(0, per, insert, 0, unroll=UNROLL)
    scores = p_s[...]
    expd = jnp.exp(scores - jnp.max(scores, axis=-1, keepdims=True))
    p_s[...] = (expd / jnp.sum(expd, axis=-1, keepdims=True)).astype(BF16).astype(F32)

    def combine(i, carry):
        probs = p_s[pl.ds(pl.multiple_of(i * heads, heads), heads), :].astype(BF16)
        outs = lax.dot_general(probs, vo_ref[0, i].reshape(rows, seq), (((1,), (1,)), ((), ())),
                               preferred_element_type=F32)
        o_s[pl.ds(i, 1), :] = jnp.sum(jnp.where(mine, outs, 0.0), axis=0, keepdims=True)
        return carry

    lax.fori_loop(0, per, combine, 0, unroll=UNROLL)
    o_ref[...] = o_s[...].astype(BF16)


def attention(layer, part, parts, hidden, gain, w_qkv, cos_t, sin_t, seq_lens, kc, vc, outs):
    layers, batch, heads, head_dim, seq = kc.shape
    rows = heads * head_dim
    count, model = hidden.shape
    per = 16
    first = part * count // per
    whole = lambda *shape: pl.BlockSpec(shape, lambda s, n: (0,) * len(shape))
    cache_block = pl.BlockSpec((1, per, heads, head_dim, seq), lambda s, n: (layer, first + s, 0, 0, 0))
    in_specs = [whole(count, model), whole(1, model),
                pl.BlockSpec((1, 3 * rows, model), lambda s, n: (layer, 0, 0)),
                whole(head_dim // 2, seq), whole(head_dim // 2, seq), cache_block, cache_block]
    args = [seq_lens, hidden, gain, w_qkv, cos_t, sin_t, kc, vc]
    aliases = {}
    if outs is not None:
        in_specs += [pl.BlockSpec(memory_space=pl.ANY)] * 2
        args += list(outs)
        aliases = {8: 1, 9: 2}
    cache_shape = jax.ShapeDtypeStruct(kc.shape, kc.dtype)
    return pl.pallas_call(
        functools.partial(attn_kernel, heads=heads, head_dim=head_dim, scale=head_dim ** -0.5, row0=part * count),
        grid_spec=pltpu.PrefetchScalarGridSpec(
            num_scalar_prefetch=1, grid=(count // per,), in_specs=in_specs,
            out_specs=[pl.BlockSpec((per, rows), lambda s, n: (s, 0)), cache_block, cache_block],
            scratch_shapes=[pltpu.VMEM((seq, rows), F32), pltpu.VMEM((rows, seq), F32),
                            pltpu.VMEM((rows, seq), F32), pltpu.VMEM((per, rows), F32),
                            pltpu.VMEM((per * heads, seq), F32)]),
        out_shape=[jax.ShapeDtypeStruct((count, rows), BF16), cache_shape, cache_shape],
        input_output_aliases=aliases,
        compiler_params=pltpu.CompilerParams(dimension_semantics=("arbitrary",), vmem_limit_bytes=48 << 20),
        cost_estimate=pl.CostEstimate(flops=30_000_000_000 // parts, bytes_accessed=kc.size * 4 // parts,
                                      transcendentals=0),
        name=f"attention_{layer}_{part}",
    )(*args)


def solution(mesh):
    cache_spec = P(None, ROW_AXES, None, "tg", None)
    in_specs = (P(ROW_AXES, None), P(ROW_AXES), cache_spec, cache_spec,
                P("pp", None), P("pp", TRAIN_AXES, None), P("pp", None, TRAIN_AXES),
                P("pp", None), P("pp", TRAIN_AXES, None), P("pp", None, TRAIN_AXES))
    out_specs = (P(ROW_AXES, None), cache_spec, cache_spec, P(None, "tg", None), P(None, "tg", None))

    def body(hidden_in, seq_lens, k_cache, v_cache, attn_gain, w_qkv, w_o, mlp_gain, w_gate_up, w_down):
        layers, batch, _, heads, head_dim = k_cache.shape
        model = hidden_in.shape[1]
        stage = lax.axis_index("pp")
        rank = lax.axis_index("tg")
        half = lax.axis_index("grp")
        groups = w_qkv.shape[1] // (3 * head_dim)
        ffn = w_gate_up.shape[1] // 2
        cols = w_o.shape[2]
        swap = lambda x, axis: lax.ppermute(x, axis, SWAP)

        def after(x, *deps):
            return lax.optimization_barrier((x,) + deps)[0]

        kc = jnp.transpose(k_cache, (0, 1, 3, 4, 2))
        vc = jnp.transpose(v_cache, (0, 1, 3, 4, 2))

        shard_qkv = w_qkv.reshape(groups, 3, head_dim, model)
        far_qkv = swap(shard_qkv, "pp")
        gains = jnp.stack([attn_gain[0], mlp_gain[0]])
        far_gains = swap(gains, "pp")
        near_qkv = swap(shard_qkv, "grp")
        shard_o = w_o[0]
        peer_o = swap(shard_o, "tg")
        near_o = swap(shard_o, "grp")
        shard_gu = w_gate_up.reshape(2, ffn, model)
        shard_down = jnp.transpose(w_down[0])
        near_gu = swap(shard_gu, "grp")
        near_down = swap(shard_down, "grp")
        peer_near_o = swap(peer_o, "grp")
        far_o = swap(after(shard_o, far_qkv), "pp")
        cos_t, sin_t = rope_tables_t(seq_lens, head_dim)

        spots = ((stage, half), (stage, 1 - half), (1 - stage, half), (1 - stage, 1 - half))
        spots = [jnp.stack(spot).astype(jnp.int32) for spot in spots]

        qkv_shape = (layers, 3, 2, groups, head_dim, model)
        qkv_spot = lambda lay, sh, t: (lay, t % 3, sh, t // 3)
        flat_qkv = lambda x: x.reshape(groups * 3, head_dim, model)
        gen_qkv = place([flat_qkv(shard_qkv), flat_qkv(near_qkv)], spots[:2], None, qkv_shape, qkv_spot)
        gu_shape = (layers, 2, 2, ffn, model)
        gen_gu = place([shard_gu, near_gu], spots[:2], None, gu_shape, lambda lay, sh, t: (lay, t, sh))
        far_qkv_in = far_qkv
        far_qkv = after(far_qkv, gen_qkv, gen_gu)
        far_near_qkv = swap(far_qkv, "grp")
        gen_qkv = place([flat_qkv(far_qkv), flat_qkv(far_near_qkv)], spots[2:], gen_qkv, qkv_shape, qkv_spot)
        gen_qkv = gen_qkv.reshape(layers, 6 * groups * head_dim, model)

        chunk = ffn // 2

        def gu_send(c, *deps):
            return swap(after(w_gate_up[0, c * chunk:(c + 1) * chunk], *deps), "pp")

        def gu_take(c, pair, dst):
            rows = [x[None] for piece in pair for x in (piece, swap(piece, "grp"))]
            for i in (0, 1):
                spot = lambda lay, sh, t: (lay, c // 2, sh, pl.ds(i * chunk, chunk))
                dst = place(rows[2 * i:2 * i + 2], spots[2:], dst, gu_shape, spot)
            return dst

        def mlp(rows_in, gain):
            normed = rms_norm(rows_in, gain)
            total = 0.0
            for gu, down in ((w_gate_up[0], shard_down), (near_gu.reshape(2 * ffn, model), near_down)):
                gate_up = jnp.einsum("bd,rd->br", normed, gu, preferred_element_type=F32)
                act = (jax.nn.silu(gate_up[:, :ffn]) * gate_up[:, ffn:]).astype(BF16)
                total = total + jnp.einsum("bf,fd->bd", act, down, preferred_element_type=F32)
            return total

        first = jnp.where(stage == 0, gains, far_gains)
        second = jnp.where(stage == 0, far_gains, gains)
        sent = [gu_send(0, far_qkv_in)]
        count = batch // PARTS
        mid = count // 2
        hidden = [hidden_in[i * count:(i + 1) * count] for i in range(PARTS)]
        caches = None
        mine_rows = lambda x: lax.dynamic_slice_in_dim(x, rank * mid, mid, 0)
        peer_rows = lambda x: lax.dynamic_slice_in_dim(x, (1 - rank) * mid, mid, 0)
        by_half = lambda x: (jnp.where(half == 0, x[:, :cols], x[:, cols:]),
                             jnp.where(half == 0, x[:, cols:], x[:, :cols]))
        for layer, gain in enumerate((first, second)):
            o_vals = []
            for i in range(PARTS):
                o_part, *caches = attention(layer, i, PARTS, hidden[i], gain[0][None], gen_qkv, cos_t, sin_t,
                                            seq_lens, kc, vc, caches)
                if layer == 0 and i == 0:
                    far_o = after(far_o, o_part)
                    far_peer_o = swap(far_o, "tg")
                    far_near_o = swap(far_o, "grp")
                    sent[0] = after(sent[0], o_part)
                    caches[0] = after(caches[0], far_o, sent[0])
                    sent.append(gu_send(1, o_part, sent[0]))
                if layer == 1 and i == 0:
                    caches[0] = after(caches[0], sent[2])
                o_vals.append(o_part)
            if layer == 0:
                stage_o = (shard_o, near_o, peer_o, peer_near_o)
                away_o = (far_o, far_near_o, far_peer_o, swap(far_peer_o, "grp"))
                stage_o, away_o = jnp.concatenate(stage_o, axis=1), jnp.concatenate(away_o, axis=1)
                layer_o = (jnp.where(stage == 0, stage_o, away_o), jnp.where(stage == 0, away_o, stage_o))
            if layer == 1:
                sent[3] = after(sent[3], o_vals[1])
                gu_pair = [after(sent[2], o_vals[1]), sent[3]]
            backs, owns = [], []
            for i in range(PARTS):
                o_peer = after(swap(o_vals[i], "tg"), o_vals[1])
                o_all = jnp.concatenate(by_half(o_vals[i]) + by_half(o_peer), axis=1)
                proj = jnp.einsum("bk,dk->bd", o_all, layer_o[layer], preferred_element_type=F32)
                hid = (hidden[i].astype(F32) + proj).astype(BF16)
                if layer == 0 and i == 0:
                    hid = after(hid, sent[1])
                away = swap(hid, "pp")
                if i:
                    away = after(away, give)
                part = mlp(jnp.concatenate([hid, away], axis=0), mlp_gain[0])
                keep = jnp.concatenate([mine_rows(part[:count]), mine_rows(part[count:])], axis=0)
                give = jnp.concatenate([peer_rows(part[:count]), peer_rows(part[count:])], axis=0)
                base = jnp.concatenate([mine_rows(hid), mine_rows(away)], axis=0).astype(F32)
                done = (base + (keep + swap(give, "tg"))).astype(BF16)
                if layer == 1 and i:
                    gen_gu = gu_take(2, gu_pair, gen_gu)
                    done = after(done, gen_gu)
                owns.append(done[:mid])
                backs.append(swap(done[mid:], "pp"))
            if layer == 0:
                sent += [gu_send(2, *backs), gu_send(3, *backs)]
            hidden = []
            for own, back in zip(owns, backs):
                block = jnp.where(stage == layer, own, back)
                other = swap(block, "tg")
                hidden.append(jnp.concatenate([jnp.where(rank == 0, block, other),
                                               jnp.where(rank == 0, other, block)], axis=0))
            if layer == 0:
                gen_gu = gu_take(0, sent[:2], gen_gu)
        hidden = jnp.concatenate(hidden, axis=0)

        restore = lambda x: jnp.transpose(x, (0, 1, 4, 2, 3))
        return (hidden, restore(caches[0]), restore(caches[1]), gen_qkv, gen_gu.reshape(layers, 4 * ffn, model))

    return jax.shard_map(body, mesh=mesh, in_specs=in_specs, out_specs=out_specs, check_vma=False)
```

```python
import functools

import jax
import jax.numpy as jnp
from jax import lax
from jax.experimental import pallas as pl
from jax.experimental.pallas import tpu as pltpu
from jax.sharding import PartitionSpec as P


ROPE_THETA = 500000.0
NORM_EPS = 1e-5
MASK_FILL = -1e30
UNROLL = 16
PARTS = 2
GU_CUTS = (17, 49, 71)
ROW_AXES = ("pp", "grp")
TRAIN_AXES = ("tg", "grp")
SWAP = ((0, 1), (1, 0))
F32 = jnp.float32
BF16 = jnp.bfloat16


def rms_norm(hidden, gain_vec):
    hidden_f32 = hidden.astype(F32)
    inv_rms = lax.rsqrt(jnp.mean(hidden_f32 * hidden_f32, axis=-1, keepdims=True) + NORM_EPS)
    return (hidden_f32 * inv_rms * gain_vec.astype(F32)).astype(BF16)


def rope_tables_t(seq_lens, head_dim):
    inv_freq = jnp.power(ROPE_THETA, -jnp.arange(0, head_dim, 2).astype(F32) / head_dim)
    angles = inv_freq[:, None] * seq_lens.astype(F32)[None, :]
    return jnp.cos(angles), jnp.sin(angles)


def place_kernel(spots_ref, *refs, count, blocks, alias):
    pieces = refs[:count]
    dst = refs[count + alias]
    bufs = refs[count + alias + 1:2 * count + alias + 1]
    sem_in, sem_out = refs[-2:]
    reads, writes = [], []
    for i, (p, src, _) in enumerate(blocks):
        reads.append(pltpu.make_async_copy(pieces[p].at[src], bufs[p].at[src], sem_in.at[i]))
        reads[-1].start()
    for i, (p, src, spot) in enumerate(blocks):
        reads[i].wait()
        target = dst.at[spot(spots_ref[p, 0], spots_ref[p, 1])]
        writes.append(pltpu.make_async_copy(bufs[p].at[src], target, sem_out.at[i]))
        writes[-1].start()
    for write in writes:
        write.wait()


def place(pieces, spots, dst, dst_shape, blocks):
    count, alias = len(pieces), int(dst is not None)
    size = sum(p.size for p in pieces)
    sems = pltpu.SemaphoreType.DMA((len(blocks),))
    return pl.pallas_call(
        functools.partial(place_kernel, count=count, blocks=blocks, alias=alias),
        in_specs=[pl.BlockSpec(memory_space=pltpu.SMEM)] + [pl.BlockSpec(memory_space=pl.ANY)] * (count + alias),
        out_specs=pl.BlockSpec(memory_space=pl.ANY),
        out_shape=jax.ShapeDtypeStruct(dst_shape, BF16),
        scratch_shapes=[pltpu.VMEM(p.shape, BF16) for p in pieces] + [sems, sems],
        input_output_aliases={count + 1: 0} if alias else {},
        compiler_params=pltpu.CompilerParams(vmem_limit_bytes=2 * size + (2 << 20)),
        cost_estimate=pl.CostEstimate(flops=size * 3000, bytes_accessed=size * 4, transcendentals=0),
        name="place",
    )(jnp.stack(spots), *pieces, *([dst] if alias else []))


def rope_t(vals, cos_t, sin_t):
    half = vals.shape[1] // 2
    lo, hi = vals[:, :half], vals[:, half:]
    return jnp.concatenate([lo * cos_t[None] - hi * sin_t[None], hi * cos_t[None] + lo * sin_t[None]], axis=1)


def project_kernel(half_ref, own_ref, away_ref, gain_ref, wa_ref, wb_ref, cos_ref, sin_ref, own_out, away_out):
    groups, _, head_dim, model = wa_ref.shape
    count = own_ref.shape[0]
    rows = groups * head_dim
    normed = rms_norm(jnp.concatenate([own_ref[...], away_ref[...]], axis=0), gain_ref[...])
    for ref, shard in ((wa_ref, half_ref[0]), (wb_ref, 1 - half_ref[0])):
        spot = pl.ds(pl.multiple_of(shard * rows, rows), rows)
        for t in range(3):
            w = ref[:, t].reshape(rows, model)
            vals = lax.dot_general(w, normed, (((1,), (1,)), ((), ())), preferred_element_type=F32)
            if t < 2:
                vals = rope_t(vals.reshape(groups, head_dim, 2 * count), cos_ref[...], sin_ref[...])
                vals = vals.reshape(rows, 2 * count)
            vals = vals.astype(BF16)
            own_out[t, spot, :] = vals[:, :count]
            away_out[t, spot, :] = vals[:, count:]


def project(half, own, away, gain, w_own, w_near, cos_t, sin_t):
    count = own.shape[0]
    out = jax.ShapeDtypeStruct((3, 2 * w_own.shape[0] * w_own.shape[2], count), BF16)
    vmem = pl.BlockSpec(memory_space=pltpu.VMEM)
    return pl.pallas_call(
        project_kernel,
        in_specs=[pl.BlockSpec(memory_space=pltpu.SMEM)] + [vmem] * 7,
        out_specs=[vmem] * 2, out_shape=[out, out],
        compiler_params=pltpu.CompilerParams(vmem_limit_bytes=24 << 20),
        cost_estimate=pl.CostEstimate(flops=3_000_000_000, bytes_accessed=w_own.size * 4, transcendentals=0),
        name="project",
    )(half, own, away, gain, w_own, w_near, cos_t, sin_t)


def mlp_kernel(rank_ref, hid_ref, away_ref, gain_ref, gu_a, gu_b, dn_a, dn_b, keep_ref, give_ref, base_ref,
               gu_s, dn_s, total, sems):
    count = hid_ref.shape[0]
    mid = count // 2
    copies = []
    for p, (gu, dn) in enumerate(((gu_a, dn_a), (gu_b, dn_b))):
        for t, (src, dst) in enumerate(((gu.at[0], gu_s.at[p, 0]), (gu.at[1], gu_s.at[p, 1]), (dn, dn_s.at[p]))):
            copies.append(pltpu.make_async_copy(src, dst, sems.at[3 * p + t]))
            copies[-1].start()
    normed = rms_norm(jnp.concatenate([hid_ref[...], away_ref[...]], axis=0), gain_ref[...])
    nt = (((1,), (1,)), ((), ()))
    for p in range(2):
        copies[3 * p].wait()
        gate = lax.dot_general(gu_s[p, 0], normed, nt, preferred_element_type=F32)
        copies[3 * p + 1].wait()
        up = lax.dot_general(gu_s[p, 1], normed, nt, preferred_element_type=F32)
        act = (jax.nn.silu(gate) * up).T.astype(BF16)
        copies[3 * p + 2].wait()
        part = jnp.dot(act, dn_s[p], preferred_element_type=F32)
        total[...] = part if p == 0 else total[...] + part
    rank = rank_ref[0]
    mine = pl.multiple_of(rank * mid, mid)
    peer = pl.multiple_of((1 - rank) * mid, mid)
    for i, ref in enumerate((hid_ref, away_ref)):
        keep_ref[i * mid:(i + 1) * mid, :] = total[pl.ds(i * count + mine, mid), :]
        give_ref[i * mid:(i + 1) * mid, :] = total[pl.ds(i * count + peer, mid), :]
        base_ref[i * mid:(i + 1) * mid, :] = ref[pl.ds(mine, mid), :]


def mlp(rank, hid, away, gain, gus, downs):
    count, model = hid.shape
    ffn = downs[0].shape[0]
    vmem, hbm = pl.BlockSpec(memory_space=pltpu.VMEM), pl.BlockSpec(memory_space=pl.ANY)
    half_f32 = jax.ShapeDtypeStruct((count, model), F32)
    return pl.pallas_call(
        mlp_kernel,
        in_specs=[pl.BlockSpec(memory_space=pltpu.SMEM)] + [vmem] * 3 + [hbm] * 4,
        out_specs=[vmem] * 3,
        out_shape=[half_f32, half_f32, jax.ShapeDtypeStruct((count, model), BF16)],
        scratch_shapes=[pltpu.VMEM((2, 2, ffn, model), BF16), pltpu.VMEM((2, ffn, model), BF16),
                        pltpu.VMEM((2 * count, model), F32), pltpu.SemaphoreType.DMA((6,))],
        compiler_params=pltpu.CompilerParams(vmem_limit_bytes=32 << 20),
        cost_estimate=pl.CostEstimate(flops=4_000_000_000, bytes_accessed=6 * ffn * model * 2, transcendentals=0),
        name="mlp",
    )(rank, hid, away, gain, *gus, *downs)


def attn_kernel(lens_ref, *rest, heads, head_dim, scale, row0, ready):
    heads_in, rest = rest[:1 if ready else 5], rest[1 if ready else 5:]
    k_ref, v_ref = rest[:2]
    o_ref, ko_ref, vo_ref, q_s, kt_s, vt_s, o_s, p_s = rest[-8:]
    rows = heads * head_dim
    per = k_ref.shape[1]
    seq = k_ref.shape[-1]
    batch = seq
    step = pl.program_id(0)

    @pl.when(step == 0)
    def _():
        if ready:
            for t, ref in enumerate((None, kt_s, vt_s)):
                vals = heads_in[0][t].astype(F32)
                if t:
                    ref[...] = vals
                else:
                    q_s[...] = vals.T
            return
        h_ref, gain_ref, w_ref, cos_ref, sin_ref = heads_in
        normed = rms_norm(h_ref[...], gain_ref[...])
        normed = jnp.concatenate([normed] * (batch // h_ref.shape[0]), axis=0)

        def proj(t, turn):
            vals = lax.dot_general(w_ref[0, t * rows:(t + 1) * rows, :], normed, (((1,), (1,)), ((), ())),
                                   preferred_element_type=F32)
            if turn:
                vals = rope_t(vals.reshape(heads, head_dim, batch), cos_ref[...], sin_ref[...])
            return vals.reshape(rows, batch).astype(BF16).astype(F32)

        q_s[...] = proj(0, True).T
        kt_s[...] = proj(1, True)
        vt_s[...] = proj(2, False)

    lane = lax.broadcasted_iota(jnp.int32, (1, seq), 1)
    head_of = lax.broadcasted_iota(jnp.int32, (heads, rows), 1) // head_dim
    mine = head_of == lax.broadcasted_iota(jnp.int32, (heads, rows), 0)

    def insert(i, carry):
        b = row0 + step * per + i
        n = lens_ref[b]
        shift = lax.rem(n - b + seq, seq)
        at_n = jnp.broadcast_to(lane == n, (rows, seq))
        k_new = pltpu.roll(kt_s[...], shift, 1).astype(BF16)
        v_new = pltpu.roll(vt_s[...], shift, 1).astype(BF16)
        k_all = jnp.where(at_n, k_new, k_ref[0, i].reshape(rows, seq))
        v_all = jnp.where(at_n, v_new, v_ref[0, i].reshape(rows, seq))
        ko_ref[0, i] = k_all.reshape(heads, head_dim, seq)
        vo_ref[0, i] = v_all.reshape(heads, head_dim, seq)
        q_diag = jnp.where(mine, q_s[pl.ds(b, 1), :], 0.0).astype(BF16)
        scores = jnp.dot(q_diag, k_all, preferred_element_type=F32) * scale
        p_s[pl.ds(pl.multiple_of(i * heads, heads), heads), :] = jnp.where(lane <= n, scores, MASK_FILL)
        return carry

    lax.fori_loop(0, per, insert, 0, unroll=UNROLL)
    scores = p_s[...]
    expd = jnp.exp(scores - jnp.max(scores, axis=-1, keepdims=True))
    p_s[...] = (expd / jnp.sum(expd, axis=-1, keepdims=True)).astype(BF16).astype(F32)

    def combine(i, carry):
        probs = p_s[pl.ds(pl.multiple_of(i * heads, heads), heads), :].astype(BF16)
        outs = lax.dot_general(probs, vo_ref[0, i].reshape(rows, seq), (((1,), (1,)), ((), ())),
                               preferred_element_type=F32)
        o_s[pl.ds(i, 1), :] = jnp.sum(jnp.where(mine, outs, 0.0), axis=0, keepdims=True)
        return carry

    lax.fori_loop(0, per, combine, 0, unroll=UNROLL)
    o_ref[...] = o_s[...].astype(BF16)


def attention(layer, part, parts, heads_in, seq_lens, kc, vc, outs):
    _, batch, heads, head_dim, seq = kc.shape
    rows = heads * head_dim
    count = batch // parts
    ready = len(heads_in) == 1
    per = 16
    first = part * count // per
    whole = lambda *shape: pl.BlockSpec(shape, lambda s, n: (0,) * len(shape))
    cache_block = pl.BlockSpec((1, per, heads, head_dim, seq), lambda s, n: (layer, first + s, 0, 0, 0))
    if ready:
        in_specs = [whole(3, rows, seq)]
    else:
        model = heads_in[0].shape[1]
        in_specs = [whole(count, model), whole(1, model), pl.BlockSpec((1, 3 * rows, model), lambda s, n: (layer, 0, 0)),
                    whole(head_dim // 2, seq), whole(head_dim // 2, seq)]
    in_specs += [cache_block, cache_block]
    args = [seq_lens, *heads_in, kc, vc]
    aliases = {}
    if outs is not None:
        in_specs += [pl.BlockSpec(memory_space=pl.ANY)] * 2
        args += list(outs)
        aliases = {len(args) - 2: 1, len(args) - 1: 2}
    cache_shape = jax.ShapeDtypeStruct(kc.shape, kc.dtype)
    return pl.pallas_call(
        functools.partial(attn_kernel, heads=heads, head_dim=head_dim, scale=head_dim ** -0.5, row0=part * count,
                          ready=ready),
        grid_spec=pltpu.PrefetchScalarGridSpec(
            num_scalar_prefetch=1, grid=(count // per,), in_specs=in_specs,
            out_specs=[pl.BlockSpec((per, rows), lambda s, n: (s, 0)), cache_block, cache_block],
            scratch_shapes=[pltpu.VMEM((seq, rows), F32), pltpu.VMEM((rows, seq), F32),
                            pltpu.VMEM((rows, seq), F32), pltpu.VMEM((per, rows), F32),
                            pltpu.VMEM((per * heads, seq), F32)]),
        out_shape=[jax.ShapeDtypeStruct((count, rows), BF16), cache_shape, cache_shape],
        input_output_aliases=aliases,
        compiler_params=pltpu.CompilerParams(dimension_semantics=("arbitrary",), vmem_limit_bytes=48 << 20),
        cost_estimate=pl.CostEstimate(flops=30_000_000_000 // parts, bytes_accessed=kc.size * 4 // parts,
                                      transcendentals=0),
    )(*args)


def solution(mesh):
    cache_spec = P(None, ROW_AXES, None, "tg", None)
    in_specs = (P(ROW_AXES, None), P(ROW_AXES), cache_spec, cache_spec,
                P("pp", None), P("pp", TRAIN_AXES, None), P("pp", None, TRAIN_AXES),
                P("pp", None), P("pp", TRAIN_AXES, None), P("pp", None, TRAIN_AXES))
    out_specs = (P(ROW_AXES, None), cache_spec, cache_spec, P(None, "tg", None), P(None, "tg", None))

    def decode(hidden_in, seq_lens, k_cache, v_cache, attn_gain, w_qkv, w_o, mlp_gain, w_gate_up, w_down):
        layers, batch, _, _, head_dim = k_cache.shape
        model = hidden_in.shape[1]
        stage = lax.axis_index("pp")
        rank = lax.axis_index("tg")
        half = lax.axis_index("grp")
        groups = w_qkv.shape[1] // (3 * head_dim)
        ffn = w_gate_up.shape[1] // 2
        cols = w_o.shape[2]

        def swap(x, axis):
            return lax.ppermute(x, axis, SWAP)

        def after(x, *deps):
            return lax.optimization_barrier((x,) + deps)[0]

        kc = jnp.transpose(k_cache, (0, 1, 3, 4, 2))
        vc = jnp.transpose(v_cache, (0, 1, 3, 4, 2))

        away_lens = swap(seq_lens, "pp")
        away_in = swap(hidden_in, "pp")
        shard_qkv = w_qkv.reshape(groups, 3, head_dim, model)
        near_qkv = swap(shard_qkv, "grp")
        gains = jnp.stack([attn_gain[0], mlp_gain[0]])
        far_gains = swap(gains, "pp")
        cos_t, sin_t = rope_tables_t(seq_lens, head_dim)
        away_cos, away_sin = rope_tables_t(away_lens, head_dim)
        heads_own, heads_away = project(
            half[None], hidden_in, away_in, attn_gain, shard_qkv, near_qkv,
            jnp.concatenate([cos_t, away_cos], axis=1), jnp.concatenate([sin_t, away_sin], axis=1))
        heads_back = swap(heads_away, "pp")

        shard_o = w_o[0]
        peer_o = swap(shard_o, "tg")
        near_o = swap(shard_o, "grp")
        shard_gu = w_gate_up.reshape(2, ffn, model)
        shard_down = jnp.transpose(w_down[0])
        near_gu = swap(shard_gu, "grp")
        near_down = swap(shard_down, "grp")
        peer_near_o = swap(peer_o, "grp")

        spots = ((stage, half), (stage, 1 - half), (1 - stage, half), (1 - stage, 1 - half))
        spots = [jnp.stack(spot).astype(jnp.int32) for spot in spots]

        qkv_shape = (layers, 3, 2, groups, head_dim, model)
        gu_shape = (layers, 2, 2, ffn, model)

        def qkv_blocks(pieces, first, many):
            return [(p, (slice(None), t), lambda lay, sh, t=t: (lay, t, sh, pl.ds(first, many)))
                    for p in range(pieces) for t in range(3)]

        def gu_blocks(pieces, lo, hi):
            blocks = []
            for p in range(pieces):
                for t in range(2):
                    a, b = max(lo, t * ffn), min(hi, (t + 1) * ffn)
                    if a < b:
                        blocks.append((p, pl.ds(a - lo, b - a), lambda lay, sh, t=t, a=a, b=b: (
                            lay, t, sh, pl.ds(a - t * ffn, b - a))))
            return blocks

        def qkv_send(i, *deps):
            many = groups // 2
            return swap(after(shard_qkv[i * many:(i + 1) * many], *deps), "pp")

        def qkv_take(i, piece, dst):
            many = groups // 2
            near = swap(piece, "grp")
            return place([piece, near], spots[2:], dst, qkv_shape, qkv_blocks(2, i * many, many))

        cuts = [0, GU_CUTS[0] * ffn // 44, GU_CUTS[1] * ffn // 44, GU_CUTS[2] * ffn // 44, 2 * ffn]

        def gu_send(c, *deps):
            return swap(after(w_gate_up[0, cuts[c]:cuts[c + 1]], *deps), "pp")

        def gu_take(c, piece, dst):
            near = swap(piece, "grp")
            return place([piece, near], spots[2:], dst, gu_shape, gu_blocks(2, cuts[c], cuts[c + 1]))

        gen_qkv = place([shard_qkv, near_qkv], spots[:2], None, qkv_shape, qkv_blocks(2, 0, groups))
        flat_gu = lambda x: x.reshape(2 * ffn, model)
        gen_gu = place([flat_gu(shard_gu), flat_gu(near_gu)], spots[:2], None, gu_shape, gu_blocks(2, 0, 2 * ffn))
        heads_in = jnp.where(stage == 0, heads_own, after(heads_back, gen_qkv, gen_gu))

        first = jnp.where(stage == 0, gains, far_gains)
        second = jnp.where(stage == 0, far_gains, gains)
        far_o = swap(after(shard_o, heads_back), "pp")
        far_heads = [qkv_send(0, heads_back)]
        count = batch // PARTS
        mid = count // 2
        hidden = [hidden_in[i * count:(i + 1) * count] for i in range(PARTS)]
        caches = None
        by_half = lambda x: (jnp.where(half == 0, x[:, :cols], x[:, cols:]),
                             jnp.where(half == 0, x[:, cols:], x[:, :cols]))
        sent = {}
        for layer, gain in enumerate((first, second)):
            o_vals = []
            for i in range(PARTS):
                vals = (heads_in,) if layer == 0 else (
                    hidden[i], gain[0][None], gen_qkv.reshape(layers, 6 * groups * head_dim, model), cos_t, sin_t)
                o_part, *caches = attention(layer, i, PARTS, vals, seq_lens, kc, vc, caches)
                if i == 0 and layer == 0:
                    far_o = after(far_o, o_part)
                    far_peer_o = swap(far_o, "tg")
                    far_near_o = swap(far_o, "grp")
                    caches[0] = after(caches[0], far_o)
                    far_heads.append(qkv_send(1, o_part))
                if i == 0 and layer == 1:
                    sent[1] = after(sent[1], o_part)
                    caches[0] = after(caches[0], sent[1])
                    sent[2] = gu_send(2, o_part)
                o_vals.append(o_part)
            if layer == 0:
                far_heads[0] = after(far_heads[0], o_vals[1])
                gen_qkv = qkv_take(0, far_heads[0], gen_qkv)
                stage_o = (shard_o, near_o, peer_o, peer_near_o)
                away_o = (far_o, far_near_o, far_peer_o, swap(far_peer_o, "grp"))
                stage_o, away_o = jnp.concatenate(stage_o, axis=1), jnp.concatenate(away_o, axis=1)
                layer_o = (jnp.where(stage == 0, stage_o, away_o), jnp.where(stage == 0, away_o, stage_o))
            if layer == 1:
                sent[2] = after(sent[2], o_vals[1])
            backs, owns = [], []
            give = None
            for i in range(PARTS):
                o_peer = after(swap(o_vals[i], "tg"), o_vals[1])
                o_all = jnp.concatenate(by_half(o_vals[i]) + by_half(o_peer), axis=1)
                proj = jnp.einsum("bk,dk->bd", o_all, layer_o[layer], preferred_element_type=F32)
                hid = (hidden[i].astype(F32) + proj).astype(BF16)
                away = swap(hid, "pp")
                if i:
                    sent[3 * layer] = gu_send(3 * layer, away)
                    away = after(away, give)
                elif layer == 0:
                    far_heads[1] = after(far_heads[1], hid)
                    away = after(away, far_heads[1])
                    gen_qkv = qkv_take(1, far_heads[1], gen_qkv)
                keep, give, base = mlp(rank[None], hid, away, mlp_gain, (shard_gu, near_gu), (shard_down, near_down))
                if i:
                    if layer == 0:
                        keep = after(keep, gen_qkv)
                    else:
                        for c in (1, 2):
                            gen_gu = gu_take(c, sent[c], gen_gu)
                        keep = after(keep, gen_gu)
                done = (base.astype(F32) + (keep + swap(give, "tg"))).astype(BF16)
                owns.append(done[:mid])
                backs.append(swap(done[mid:], "pp"))
            if layer == 0:
                sent[1] = gu_send(1, *backs)
                gen_gu = gu_take(0, sent[0], gen_gu)
            hidden = []
            for own, back in zip(owns, backs):
                block = jnp.where(stage == layer, own, back)
                other = swap(block, "tg")
                hidden.append(jnp.concatenate([jnp.where(rank == 0, block, other),
                                               jnp.where(rank == 0, other, block)], axis=0))
        gen_gu = gu_take(3, sent[3], gen_gu)
        hidden = jnp.concatenate(hidden, axis=0)
        gen_qkv = gen_qkv.reshape(layers, 6 * groups * head_dim, model)

        restore = lambda x: jnp.transpose(x, (0, 1, 4, 2, 3))
        return (hidden, restore(caches[0]), restore(caches[1]), gen_qkv, gen_gu.reshape(layers, 4 * ffn, model))

    return jax.shard_map(decode, mesh=mesh, in_specs=in_specs, out_specs=out_specs, check_vma=False)
```

```python
import functools

import jax
import jax.numpy as jnp
from jax import lax
from jax.experimental import pallas as pl
from jax.experimental.pallas import tpu as pltpu
from jax.sharding import PartitionSpec as P


ROPE_THETA = 500000.0
NORM_EPS = 1e-5
MASK_FILL = -1e30
UNROLL = 16
PARTS = 2
GU_CUTS = (17, 49, 71)
ROW_AXES = ("pp", "grp")
TRAIN_AXES = ("tg", "grp")
SWAP = ((0, 1), (1, 0))
F32 = jnp.float32
BF16 = jnp.bfloat16


def rms_norm(hidden, gain_vec):
    hidden_f32 = hidden.astype(F32)
    inv_rms = lax.rsqrt(jnp.mean(hidden_f32 * hidden_f32, axis=-1, keepdims=True) + NORM_EPS)
    return (hidden_f32 * inv_rms * gain_vec.astype(F32)).astype(BF16)


def rope_tables_t(seq_lens, head_dim):
    inv_freq = jnp.power(ROPE_THETA, -jnp.arange(0, head_dim, 2).astype(F32) / head_dim)
    angles = inv_freq[:, None] * seq_lens.astype(F32)[None, :]
    return jnp.cos(angles), jnp.sin(angles)


def place_kernel(spots_ref, *refs, count, blocks, alias):
    pieces = refs[:count]
    dst = refs[count + alias]
    bufs = refs[count + alias + 1:2 * count + alias + 1]
    sem_in, sem_out = refs[-2:]
    reads, writes = [], []
    for i, (p, src, _) in enumerate(blocks):
        reads.append(pltpu.make_async_copy(pieces[p].at[src], bufs[p].at[src], sem_in.at[i]))
        reads[-1].start()
    for i, (p, src, spot) in enumerate(blocks):
        reads[i].wait()
        target = dst.at[spot(spots_ref[p, 0], spots_ref[p, 1])]
        writes.append(pltpu.make_async_copy(bufs[p].at[src], target, sem_out.at[i]))
        writes[-1].start()
    for write in writes:
        write.wait()


def place(pieces, spots, dst, dst_shape, blocks):
    count, alias = len(pieces), int(dst is not None)
    size = sum(p.size for p in pieces)
    sems = pltpu.SemaphoreType.DMA((len(blocks),))
    return pl.pallas_call(
        functools.partial(place_kernel, count=count, blocks=blocks, alias=alias),
        in_specs=[pl.BlockSpec(memory_space=pltpu.SMEM)] + [pl.BlockSpec(memory_space=pl.ANY)] * (count + alias),
        out_specs=pl.BlockSpec(memory_space=pl.ANY),
        out_shape=jax.ShapeDtypeStruct(dst_shape, BF16),
        scratch_shapes=[pltpu.VMEM(p.shape, BF16) for p in pieces] + [sems, sems],
        input_output_aliases={count + 1: 0} if alias else {},
        compiler_params=pltpu.CompilerParams(vmem_limit_bytes=2 * size + (2 << 20)),
        cost_estimate=pl.CostEstimate(flops=size * 3000, bytes_accessed=size * 4, transcendentals=0),
        name="place",
    )(jnp.stack(spots), *pieces, *([dst] if alias else []))


def rope_t(vals, cos_t, sin_t):
    half = vals.shape[1] // 2
    lo, hi = vals[:, :half], vals[:, half:]
    return jnp.concatenate([lo * cos_t[None] - hi * sin_t[None], hi * cos_t[None] + lo * sin_t[None]], axis=1)


def project_kernel(half_ref, own_ref, away_ref, gain_ref, wa_ref, wb_ref, cos_ref, sin_ref, own_out, away_out):
    groups, _, head_dim, model = wa_ref.shape
    count = own_ref.shape[0]
    rows = groups * head_dim
    normed = rms_norm(jnp.concatenate([own_ref[...], away_ref[...]], axis=0), gain_ref[...])
    for ref, shard in ((wa_ref, half_ref[0]), (wb_ref, 1 - half_ref[0])):
        spot = pl.ds(pl.multiple_of(shard * rows, rows), rows)
        for t in range(3):
            w = ref[:, t].reshape(rows, model)
            vals = lax.dot_general(w, normed, (((1,), (1,)), ((), ())), preferred_element_type=F32)
            if t < 2:
                vals = rope_t(vals.reshape(groups, head_dim, 2 * count), cos_ref[...], sin_ref[...])
                vals = vals.reshape(rows, 2 * count)
            vals = vals.astype(BF16)
            own_out[t, spot, :] = vals[:, :count]
            away_out[t, spot, :] = vals[:, count:]


def project(half, own, away, gain, w_own, w_near, cos_t, sin_t):
    count = own.shape[0]
    out = jax.ShapeDtypeStruct((3, 2 * w_own.shape[0] * w_own.shape[2], count), BF16)
    vmem = pl.BlockSpec(memory_space=pltpu.VMEM)
    return pl.pallas_call(
        project_kernel,
        in_specs=[pl.BlockSpec(memory_space=pltpu.SMEM)] + [vmem] * 7,
        out_specs=[vmem] * 2, out_shape=[out, out],
        compiler_params=pltpu.CompilerParams(vmem_limit_bytes=24 << 20),
        cost_estimate=pl.CostEstimate(flops=3_000_000_000, bytes_accessed=w_own.size * 4, transcendentals=0),
        name="project",
    )(half, own, away, gain, w_own, w_near, cos_t, sin_t)


def mlp_kernel(rank_ref, hid_ref, away_ref, gain_ref, gu_a, gu_b, dn_a, dn_b, keep_ref, give_ref, base_ref, total):
    count = hid_ref.shape[0]
    mid = count // 2
    normed = rms_norm(jnp.concatenate([hid_ref[...], away_ref[...]], axis=0), gain_ref[...])
    nt = (((1,), (1,)), ((), ()))
    for gu, dn in ((gu_a, dn_a), (gu_b, dn_b)):
        gate = lax.dot_general(gu[0], normed, nt, preferred_element_type=F32)
        up = lax.dot_general(gu[1], normed, nt, preferred_element_type=F32)
        act = (jax.nn.silu(gate) * up).T.astype(BF16)
        part = jnp.dot(act, dn[...], preferred_element_type=F32)
        total[...] = part if dn is dn_a else total[...] + part
    rank = rank_ref[0]
    mine = pl.multiple_of(rank * mid, mid)
    peer = pl.multiple_of((1 - rank) * mid, mid)
    for i, ref in enumerate((hid_ref, away_ref)):
        keep_ref[i * mid:(i + 1) * mid, :] = total[pl.ds(i * count + mine, mid), :]
        give_ref[i * mid:(i + 1) * mid, :] = total[pl.ds(i * count + peer, mid), :]
        base_ref[i * mid:(i + 1) * mid, :] = ref[pl.ds(mine, mid), :]


def mlp(rank, hid, away, gain, gus, downs):
    count, model = hid.shape
    ffn = downs[0].shape[0]
    vmem = pl.BlockSpec(memory_space=pltpu.VMEM)
    half_f32 = jax.ShapeDtypeStruct((count, model), F32)
    return pl.pallas_call(
        mlp_kernel,
        in_specs=[pl.BlockSpec(memory_space=pltpu.SMEM)] + [vmem] * 7,
        out_specs=[vmem] * 3,
        out_shape=[half_f32, half_f32, jax.ShapeDtypeStruct((count, model), BF16)],
        scratch_shapes=[pltpu.VMEM((2 * count, model), F32)],
        compiler_params=pltpu.CompilerParams(vmem_limit_bytes=32 << 20),
        cost_estimate=pl.CostEstimate(flops=4_000_000_000, bytes_accessed=6 * ffn * model * 2, transcendentals=0),
        name="mlp",
    )(rank, hid, away, gain, *gus, *downs)


def attn_kernel(lens_ref, *rest, heads, head_dim, scale, row0, ready, layer):
    heads_in, rest = rest[:1 if ready else 5], rest[1 if ready else 5:]
    k_ref, v_ref = rest[:2]
    if not ready:
        w_s, w_sem = rest[-2:]
        rest = rest[:-2]
    o_ref, ko_ref, vo_ref, q_s, kt_s, vt_s, o_s, p_s = rest[-8:]
    rows = heads * head_dim
    per = k_ref.shape[1]
    seq = k_ref.shape[-1]
    batch = seq
    step = pl.program_id(0)

    @pl.when(step == 0)
    def _():
        if ready:
            for t, ref in enumerate((None, kt_s, vt_s)):
                vals = heads_in[0][t].astype(F32)
                if t:
                    ref[...] = vals
                else:
                    q_s[...] = vals.T
            return
        h_ref, gain_ref, w_ref, cos_ref, sin_ref = heads_in
        fetch = pltpu.make_async_copy(w_ref.at[layer], w_s, w_sem)
        fetch.start()
        normed = rms_norm(h_ref[...], gain_ref[...])
        normed = jnp.concatenate([normed] * (batch // h_ref.shape[0]), axis=0)

        fetch.wait()

        def proj(t, turn):
            vals = lax.dot_general(w_s[t * rows:(t + 1) * rows, :], normed, (((1,), (1,)), ((), ())),
                                   preferred_element_type=F32)
            if turn:
                vals = rope_t(vals.reshape(heads, head_dim, batch), cos_ref[...], sin_ref[...])
            return vals.reshape(rows, batch).astype(BF16).astype(F32)

        q_s[...] = proj(0, True).T
        kt_s[...] = proj(1, True)
        vt_s[...] = proj(2, False)

    lane = lax.broadcasted_iota(jnp.int32, (1, seq), 1)
    head_of = lax.broadcasted_iota(jnp.int32, (heads, rows), 1) // head_dim
    mine = head_of == lax.broadcasted_iota(jnp.int32, (heads, rows), 0)

    def insert(i, carry):
        b = row0 + step * per + i
        n = lens_ref[b]
        shift = lax.rem(n - b + seq, seq)
        at_n = jnp.broadcast_to(lane == n, (rows, seq))
        k_new = pltpu.roll(kt_s[...], shift, 1).astype(BF16)
        v_new = pltpu.roll(vt_s[...], shift, 1).astype(BF16)
        k_all = jnp.where(at_n, k_new, k_ref[0, i].reshape(rows, seq))
        v_all = jnp.where(at_n, v_new, v_ref[0, i].reshape(rows, seq))
        ko_ref[0, i] = k_all.reshape(heads, head_dim, seq)
        vo_ref[0, i] = v_all.reshape(heads, head_dim, seq)
        q_diag = jnp.where(mine, q_s[pl.ds(b, 1), :], 0.0).astype(BF16)
        scores = jnp.dot(q_diag, k_all, preferred_element_type=F32) * scale
        p_s[pl.ds(pl.multiple_of(i * heads, heads), heads), :] = jnp.where(lane <= n, scores, MASK_FILL)
        return carry

    lax.fori_loop(0, per, insert, 0, unroll=UNROLL)
    scores = p_s[...]
    expd = jnp.exp(scores - jnp.max(scores, axis=-1, keepdims=True))
    p_s[...] = (expd / jnp.sum(expd, axis=-1, keepdims=True)).astype(BF16).astype(F32)

    def combine(i, carry):
        probs = p_s[pl.ds(pl.multiple_of(i * heads, heads), heads), :].astype(BF16)
        outs = lax.dot_general(probs, vo_ref[0, i].reshape(rows, seq), (((1,), (1,)), ((), ())),
                               preferred_element_type=F32)
        o_s[pl.ds(i, 1), :] = jnp.sum(jnp.where(mine, outs, 0.0), axis=0, keepdims=True)
        return carry

    lax.fori_loop(0, per, combine, 0, unroll=UNROLL)
    o_ref[...] = o_s[...].astype(BF16)


def attention(layer, part, parts, heads_in, seq_lens, kc, vc, outs):
    _, batch, heads, head_dim, seq = kc.shape
    rows = heads * head_dim
    count = batch // parts
    ready = len(heads_in) == 1
    per = 16
    first = part * count // per
    whole = lambda *shape: pl.BlockSpec(shape, lambda s, n: (0,) * len(shape))
    cache_block = pl.BlockSpec((1, per, heads, head_dim, seq), lambda s, n: (layer, first + s, 0, 0, 0))
    if ready:
        in_specs = [whole(3, rows, seq)]
    else:
        model = heads_in[0].shape[1]
        in_specs = [whole(count, model), whole(1, model), pl.BlockSpec(memory_space=pltpu.HBM),
                    whole(head_dim // 2, seq), whole(head_dim // 2, seq)]
    in_specs += [cache_block, cache_block]
    args = [seq_lens, *heads_in, kc, vc]
    aliases = {}
    if outs is not None:
        in_specs += [pl.BlockSpec(memory_space=pl.ANY)] * 2
        args += list(outs)
        aliases = {len(args) - 2: 1, len(args) - 1: 2}
    cache_shape = jax.ShapeDtypeStruct(kc.shape, kc.dtype)
    return pl.pallas_call(
        functools.partial(attn_kernel, heads=heads, head_dim=head_dim, scale=head_dim ** -0.5, row0=part * count,
                          ready=ready, layer=layer),
        grid_spec=pltpu.PrefetchScalarGridSpec(
            num_scalar_prefetch=1, grid=(count // per,), in_specs=in_specs,
            out_specs=[pl.BlockSpec((per, rows), lambda s, n: (s, 0)), cache_block, cache_block],
            scratch_shapes=[pltpu.VMEM((seq, rows), F32), pltpu.VMEM((rows, seq), F32),
                            pltpu.VMEM((rows, seq), F32), pltpu.VMEM((per, rows), F32),
                            pltpu.VMEM((per * heads, seq), F32)] + ([] if ready else [
                                pltpu.VMEM((3 * rows, heads_in[0].shape[1]), BF16), pltpu.SemaphoreType.DMA])),
        out_shape=[jax.ShapeDtypeStruct((count, rows), BF16), cache_shape, cache_shape],
        input_output_aliases=aliases,
        compiler_params=pltpu.CompilerParams(dimension_semantics=("arbitrary",), vmem_limit_bytes=28 << 20),
        cost_estimate=pl.CostEstimate(flops=30_000_000_000 // parts, bytes_accessed=kc.size * 4 // parts,
                                      transcendentals=0),
    )(*args)


def solution(mesh):
    cache_spec = P(None, ROW_AXES, None, "tg", None)
    in_specs = (P(ROW_AXES, None), P(ROW_AXES), cache_spec, cache_spec,
                P("pp", None), P("pp", TRAIN_AXES, None), P("pp", None, TRAIN_AXES),
                P("pp", None), P("pp", TRAIN_AXES, None), P("pp", None, TRAIN_AXES))
    out_specs = (P(ROW_AXES, None), cache_spec, cache_spec, P(None, "tg", None), P(None, "tg", None))

    def decode(hidden_in, seq_lens, k_cache, v_cache, attn_gain, w_qkv, w_o, mlp_gain, w_gate_up, w_down):
        layers, batch, _, _, head_dim = k_cache.shape
        model = hidden_in.shape[1]
        stage = lax.axis_index("pp")
        rank = lax.axis_index("tg")
        half = lax.axis_index("grp")
        groups = w_qkv.shape[1] // (3 * head_dim)
        ffn = w_gate_up.shape[1] // 2
        cols = w_o.shape[2]

        def swap(x, axis):
            return lax.ppermute(x, axis, SWAP)

        def after(x, *deps):
            return lax.optimization_barrier((x,) + deps)[0]

        kc = jnp.transpose(k_cache, (0, 1, 3, 4, 2))
        vc = jnp.transpose(v_cache, (0, 1, 3, 4, 2))

        away_lens = swap(seq_lens, "pp")
        away_in = swap(hidden_in, "pp")
        shard_qkv = w_qkv.reshape(groups, 3, head_dim, model)
        near_qkv = swap(shard_qkv, "grp")
        gains = jnp.stack([attn_gain[0], mlp_gain[0]])
        far_gains = swap(gains, "pp")
        cos_t, sin_t = rope_tables_t(seq_lens, head_dim)
        away_cos, away_sin = rope_tables_t(away_lens, head_dim)
        heads_own, heads_away = project(
            half[None], hidden_in, away_in, attn_gain, shard_qkv, near_qkv,
            jnp.concatenate([cos_t, away_cos], axis=1), jnp.concatenate([sin_t, away_sin], axis=1))
        heads_back = swap(heads_away, "pp")

        shard_o = w_o[0]
        peer_o = swap(shard_o, "tg")
        near_o = swap(shard_o, "grp")
        shard_gu = w_gate_up.reshape(2, ffn, model)
        shard_down = jnp.transpose(w_down[0])
        near_gu = swap(shard_gu, "grp")
        near_down = swap(shard_down, "grp")
        peer_near_o = swap(peer_o, "grp")

        spots = ((stage, half), (stage, 1 - half), (1 - stage, half), (1 - stage, 1 - half))
        spots = [jnp.stack(spot).astype(jnp.int32) for spot in spots]

        qkv_shape = (layers, 3, 2, groups, head_dim, model)
        gu_shape = (layers, 2, 2, ffn, model)

        def qkv_blocks(pieces, first, many):
            return [(p, (slice(None), t), lambda lay, sh, t=t: (lay, t, sh, pl.ds(first, many)))
                    for p in range(pieces) for t in range(3)]

        def gu_blocks(pieces, lo, hi):
            blocks = []
            for p in range(pieces):
                for t in range(2):
                    a, b = max(lo, t * ffn), min(hi, (t + 1) * ffn)
                    if a < b:
                        blocks.append((p, pl.ds(a - lo, b - a), lambda lay, sh, t=t, a=a, b=b: (
                            lay, t, sh, pl.ds(a - t * ffn, b - a))))
            return blocks

        def qkv_send(i, *deps):
            many = groups // 2
            return swap(after(late_qkv[i * many:(i + 1) * many], *deps), "pp")

        def qkv_take(i, piece, dst):
            many = groups // 2
            near = swap(piece, "grp")
            return place([piece, near], spots[2:], dst, qkv_shape, qkv_blocks(2, i * many, many))

        late_gu = after(w_gate_up[0], heads_own)
        late_qkv = after(shard_qkv, heads_own)
        cuts = [0, GU_CUTS[0] * ffn // 44, GU_CUTS[1] * ffn // 44, GU_CUTS[2] * ffn // 44, 2 * ffn]

        def gu_send(c, *deps):
            return swap(after(late_gu[cuts[c]:cuts[c + 1]], *deps), "pp")

        def gu_take(c, piece, dst):
            near = swap(piece, "grp")
            return place([piece, near], spots[2:], dst, gu_shape, gu_blocks(2, cuts[c], cuts[c + 1]))

        flat_gu = lambda x: x.reshape(2 * ffn, model)
        gen_qkv = place([shard_qkv, near_qkv], spots[:2], None, qkv_shape, qkv_blocks(2, 0, groups))
        gen_gu = place([flat_gu(shard_gu), flat_gu(near_gu)], spots[:2], None, gu_shape, gu_blocks(2, 0, 2 * ffn))
        heads_in = jnp.where(stage == 0, heads_own, after(heads_back, gen_qkv, gen_gu))

        first = jnp.where(stage == 0, gains, far_gains)
        second = jnp.where(stage == 0, far_gains, gains)
        far_o = swap(after(shard_o, heads_back), "pp")
        far_heads = [qkv_send(0, heads_back)]
        count = batch // PARTS
        mid = count // 2
        hidden = [hidden_in[i * count:(i + 1) * count] for i in range(PARTS)]
        caches = None
        by_half = lambda x: (jnp.where(half == 0, x[:, :cols], x[:, cols:]),
                             jnp.where(half == 0, x[:, cols:], x[:, :cols]))
        sent = {}
        for layer, gain in enumerate((first, second)):
            o_vals = []
            for i in range(PARTS):
                vals = (heads_in,) if layer == 0 else (
                    hidden[i], gain[0][None], gen_qkv.reshape(layers, 6 * groups * head_dim, model), cos_t, sin_t)
                o_part, *caches = attention(layer, i, PARTS, vals, seq_lens, kc, vc, caches)
                if i == 0 and layer == 0:
                    far_o = after(far_o, o_part)
                    far_peer_o = swap(far_o, "tg")
                    far_near_o = swap(far_o, "grp")
                    caches[0] = after(caches[0], far_o)
                    far_heads.append(qkv_send(1, o_part))
                if i == 0 and layer == 1:
                    sent[0] = after(sent[0], o_part)
                    sent[2] = gu_send(2, o_part)
                    sent[3] = gu_send(3, o_part)
                o_vals.append(o_part)
            if layer == 0:
                far_heads[0] = after(far_heads[0], o_vals[1])
                gen_qkv = qkv_take(0, far_heads[0], gen_qkv)
                stage_o = (shard_o, near_o, peer_o, peer_near_o)
                away_o = (far_o, far_near_o, far_peer_o, swap(far_peer_o, "grp"))
                all_o = jnp.stack([jnp.concatenate(stage_o, axis=1), jnp.concatenate(away_o, axis=1)])
                layer_o = [lax.dynamic_index_in_dim(all_o, jnp.abs(stage - n), 0, False) for n in range(layers)]
            if layer == 1:
                for c in (1, 2, 3):
                    sent[c] = after(sent[c], o_vals[1])
            backs, owns = [], []
            give = None
            for i in range(PARTS):
                o_peer = after(swap(o_vals[i], "tg"), o_vals[1])
                o_all = jnp.concatenate(by_half(o_vals[i]) + by_half(o_peer), axis=1)
                proj = jnp.einsum("bk,dk->bd", o_all, layer_o[layer], preferred_element_type=F32)
                hid = (hidden[i].astype(F32) + proj).astype(BF16)
                away = swap(hid, "pp")
                if i:
                    if layer == 0:
                        sent[0] = gu_send(0, away)
                    away = after(away, give)
                elif layer == 0:
                    far_heads[1] = after(far_heads[1], hid)
                    away = after(away, far_heads[1])
                    gen_qkv = qkv_take(1, far_heads[1], gen_qkv)
                keep, give, base = mlp(rank[None], hid, away, mlp_gain, (shard_gu, near_gu), (shard_down, near_down))
                if i:
                    if layer == 0:
                        keep = after(keep, gen_qkv)
                    else:
                        for c in range(4):
                            gen_gu = gu_take(c, sent[c], gen_gu)
                        keep = after(keep, gen_gu)
                done = (base.astype(F32) + (keep + swap(give, "tg"))).astype(BF16)
                owns.append(done[:mid])
                backs.append(swap(done[mid:], "pp"))
            if layer == 0:
                sent[1] = gu_send(1, *backs)
            hidden = []
            for own, back in zip(owns, backs):
                block = jnp.where(stage == layer, own, back)
                other = swap(block, "tg")
                hidden.append(jnp.concatenate([jnp.where(rank == 0, block, other),
                                               jnp.where(rank == 0, other, block)], axis=0))
        hidden = jnp.concatenate(hidden, axis=0)
        gen_qkv = gen_qkv.reshape(layers, 6 * groups * head_dim, model)

        restore = lambda x: jnp.transpose(x, (0, 1, 4, 2, 3))
        return (hidden, restore(caches[0]), restore(caches[1]), gen_qkv, gen_gu.reshape(layers, 4 * ffn, model))

    return jax.shard_map(decode, mesh=mesh, in_specs=in_specs, out_specs=out_specs, check_vma=False)
```

```python
import functools

import jax
import jax.numpy as jnp
from jax import lax
from jax.experimental import pallas as pl
from jax.experimental.pallas import tpu as pltpu
from jax.sharding import PartitionSpec as P


ROPE_THETA = 500000.0
NORM_EPS = 1e-5
MASK_FILL = -1e30
UNROLL = 16
PARTS = 2
GU_CUTS = (0, 10, 26, 50, 72, 88)
ROW_AXES = ("pp", "grp")
TRAIN_AXES = ("tg", "grp")
SWAP = ((0, 1), (1, 0))
F32 = jnp.float32
BF16 = jnp.bfloat16


def rms_norm(hidden, gain_vec):
    hidden_f32 = hidden.astype(F32)
    inv_rms = lax.rsqrt(jnp.mean(hidden_f32 * hidden_f32, axis=-1, keepdims=True) + NORM_EPS)
    return (hidden_f32 * inv_rms * gain_vec.astype(F32)).astype(BF16)


def rope_tables_t(seq_lens, head_dim):
    inv_freq = jnp.power(ROPE_THETA, -jnp.arange(0, head_dim, 2).astype(F32) / head_dim)
    angles = inv_freq[:, None] * seq_lens.astype(F32)[None, :]
    return jnp.cos(angles), jnp.sin(angles)


def place_kernel(spots_ref, *refs, count, blocks, alias):
    pieces = refs[:count]
    dst = refs[count + alias]
    bufs = refs[count + alias + 1:2 * count + alias + 1]
    sem_in, sem_out = refs[-2:]
    reads, writes = [], []
    for i, (p, src, _) in enumerate(blocks):
        reads.append(pltpu.make_async_copy(pieces[p].at[src], bufs[p].at[src], sem_in.at[i]))
        reads[-1].start()
    for i, (p, src, spot) in enumerate(blocks):
        reads[i].wait()
        target = dst.at[spot(spots_ref[p, 0], spots_ref[p, 1])]
        writes.append(pltpu.make_async_copy(bufs[p].at[src], target, sem_out.at[i]))
        writes[-1].start()
    for write in writes:
        write.wait()


def place(pieces, spots, dst, dst_shape, blocks):
    count, alias = len(pieces), int(dst is not None)
    size = sum(p.size for p in pieces)
    sems = pltpu.SemaphoreType.DMA((len(blocks),))
    return pl.pallas_call(
        functools.partial(place_kernel, count=count, blocks=blocks, alias=alias),
        in_specs=[pl.BlockSpec(memory_space=pltpu.SMEM)] + [pl.BlockSpec(memory_space=pl.ANY)] * (count + alias),
        out_specs=pl.BlockSpec(memory_space=pl.ANY),
        out_shape=jax.ShapeDtypeStruct(dst_shape, BF16),
        scratch_shapes=[pltpu.VMEM(p.shape, BF16) for p in pieces] + [sems, sems],
        input_output_aliases={count + 1: 0} if alias else {},
        compiler_params=pltpu.CompilerParams(vmem_limit_bytes=2 * size + (2 << 20)),
        cost_estimate=pl.CostEstimate(flops=size * 3000, bytes_accessed=size * 4, transcendentals=0),
        name="place",
    )(jnp.stack(spots), *pieces, *([dst] if alias else []))


def rope_t(vals, cos_t, sin_t):
    half = vals.shape[1] // 2
    lo, hi = vals[:, :half], vals[:, half:]
    return jnp.concatenate([lo * cos_t[None] - hi * sin_t[None], hi * cos_t[None] + lo * sin_t[None]], axis=1)


def project_kernel(half_ref, own_ref, away_ref, gain_ref, wa_ref, wb_ref, cos_ref, sin_ref, own_out, away_out):
    groups, _, head_dim, model = wa_ref.shape
    count = own_ref.shape[0]
    rows = groups * head_dim
    normed = rms_norm(jnp.concatenate([own_ref[...], away_ref[...]], axis=0), gain_ref[...])
    for ref, shard in ((wa_ref, half_ref[0]), (wb_ref, 1 - half_ref[0])):
        spot = pl.ds(pl.multiple_of(shard * rows, rows), rows)
        for t in range(3):
            w = ref[:, t].reshape(rows, model)
            vals = lax.dot_general(w, normed, (((1,), (1,)), ((), ())), preferred_element_type=F32)
            if t < 2:
                vals = rope_t(vals.reshape(groups, head_dim, 2 * count), cos_ref[...], sin_ref[...])
                vals = vals.reshape(rows, 2 * count)
            vals = vals.astype(BF16)
            own_out[t, spot, :] = vals[:, :count]
            away_out[t, spot, :] = vals[:, count:]


def project(half, own, away, gain, w_own, w_near, cos_t, sin_t):
    count = own.shape[0]
    out = jax.ShapeDtypeStruct((3, 2 * w_own.shape[0] * w_own.shape[2], count), BF16)
    vmem = pl.BlockSpec(memory_space=pltpu.VMEM)
    return pl.pallas_call(
        project_kernel,
        in_specs=[pl.BlockSpec(memory_space=pltpu.SMEM)] + [vmem] * 7,
        out_specs=[vmem] * 2, out_shape=[out, out],
        compiler_params=pltpu.CompilerParams(vmem_limit_bytes=24 << 20),
        cost_estimate=pl.CostEstimate(flops=3_000_000_000, bytes_accessed=w_own.size * 4, transcendentals=0),
        name="project",
    )(half, own, away, gain, w_own, w_near, cos_t, sin_t)


def block_kernel(place_ref, o_own, o_own_peer, o_away, o_away_peer, hid_ref, away_ref, gain_ref, wo_a, wo_b, wo_c, wo_d,
                 gu_a, gu_b, dn_a, dn_b, keep_ref, give_ref, base_ref, total, rows_s):
    count = hid_ref.shape[0]
    mid = count // 2
    cols = wo_a.shape[1]
    rank, half = place_ref[0], place_ref[1]
    nt = (((1,), (1,)), ((), ()))
    proj = jnp.concatenate([hid_ref[...], away_ref[...]], axis=0).astype(F32)
    out = None
    for (own, away), (near, far) in (((o_own, o_away), (wo_a, wo_b)), ((o_own_peer, o_away_peer), (wo_c, wo_d))):
        o_vals = jnp.concatenate([own[...], away[...]], axis=0).astype(F32)
        lo, hi = o_vals[:, :cols], o_vals[:, cols:]
        mine = jnp.where(half == 0, lo, hi).astype(BF16)
        other = jnp.where(half == 0, hi, lo).astype(BF16)
        for vals, w in ((mine, near), (other, far)):
            part = lax.dot_general(vals, w[...], nt, preferred_element_type=F32)
            out = part if out is None else out + part
    rows = (proj + out).astype(BF16)
    rows_s[...] = rows.astype(F32)
    normed = rms_norm(rows, gain_ref[...])
    for gu, dn in ((gu_a, dn_a), (gu_b, dn_b)):
        gate = lax.dot_general(gu[0], normed, nt, preferred_element_type=F32)
        up = lax.dot_general(gu[1], normed, nt, preferred_element_type=F32)
        act = (jax.nn.silu(gate) * up).T.astype(BF16)
        part = jnp.dot(act, dn[...], preferred_element_type=F32)
        total[...] = part if dn is dn_a else total[...] + part
    mine = pl.multiple_of(rank * mid, mid)
    peer = pl.multiple_of((1 - rank) * mid, mid)
    for i in range(2):
        keep_ref[i * mid:(i + 1) * mid, :] = total[pl.ds(i * count + mine, mid), :]
        give_ref[i * mid:(i + 1) * mid, :] = total[pl.ds(i * count + peer, mid), :]
        base_ref[i * mid:(i + 1) * mid, :] = rows_s[pl.ds(i * count + mine, mid), :].astype(BF16)


def block(spot, o_vals, hid, away, gain, w_o, gus, downs):
    count, model = hid.shape
    ffn = downs[0].shape[0]
    vmem = pl.BlockSpec(memory_space=pltpu.VMEM)
    half_f32 = jax.ShapeDtypeStruct((count, model), F32)
    return pl.pallas_call(
        block_kernel,
        in_specs=[pl.BlockSpec(memory_space=pltpu.SMEM)] + [vmem] * 15,
        out_specs=[vmem] * 3,
        out_shape=[half_f32, half_f32, jax.ShapeDtypeStruct((count, model), BF16)],
        scratch_shapes=[pltpu.VMEM((2 * count, model), F32)] * 2,
        compiler_params=pltpu.CompilerParams(vmem_limit_bytes=32 << 20),
        cost_estimate=pl.CostEstimate(flops=4_000_000_000, bytes_accessed=6 * ffn * model * 2, transcendentals=0),
        name="block",
    )(spot, *o_vals, hid, away, gain, *w_o, *gus, *downs)


def attn_kernel(lens_ref, *rest, heads, head_dim, scale, row0, ready, layer):
    heads_in, rest = rest[:1 if ready else 5], rest[1 if ready else 5:]
    k_ref, v_ref = rest[:2]
    if not ready:
        w_s, w_sem = rest[-2:]
        rest = rest[:-8] + rest[-7:-2]
    o_ref, ko_ref, vo_ref, q_s, kt_s, vt_s, o_s, p_s = rest[-8:]
    rows = heads * head_dim
    per = k_ref.shape[1]
    seq = k_ref.shape[-1]
    batch = seq
    step = pl.program_id(0)

    @pl.when(step == 0)
    def _():
        if ready:
            for t, ref in enumerate((None, kt_s, vt_s)):
                vals = heads_in[0][t].astype(F32)
                if t:
                    ref[...] = vals
                else:
                    q_s[...] = vals.T
            return
        h_ref, gain_ref, w_ref, cos_ref, sin_ref = heads_in
        fetch = pltpu.make_async_copy(w_ref.at[layer], w_s, w_sem)
        fetch.start()
        normed = rms_norm(h_ref[...], gain_ref[...])
        normed = jnp.concatenate([normed] * (batch // h_ref.shape[0]), axis=0)

        fetch.wait()

        def proj(t, turn):
            vals = lax.dot_general(w_s[t * rows:(t + 1) * rows, :], normed, (((1,), (1,)), ((), ())),
                                   preferred_element_type=F32)
            if turn:
                vals = rope_t(vals.reshape(heads, head_dim, batch), cos_ref[...], sin_ref[...])
            return vals.reshape(rows, batch).astype(BF16).astype(F32)

        q_s[...] = proj(0, True).T
        kt_s[...] = proj(1, True)
        vt_s[...] = proj(2, False)

    lane = lax.broadcasted_iota(jnp.int32, (1, seq), 1)
    head_of = lax.broadcasted_iota(jnp.int32, (heads, rows), 1) // head_dim
    mine = head_of == lax.broadcasted_iota(jnp.int32, (heads, rows), 0)

    def insert(i, carry):
        b = row0 + step * per + i
        n = lens_ref[b]
        shift = lax.rem(n - b + seq, seq)
        at_n = jnp.broadcast_to(lane == n, (rows, seq))
        k_new = pltpu.roll(kt_s[...], shift, 1).astype(BF16)
        v_new = pltpu.roll(vt_s[...], shift, 1).astype(BF16)
        k_all = jnp.where(at_n, k_new, k_ref[0, i].reshape(rows, seq))
        v_all = jnp.where(at_n, v_new, v_ref[0, i].reshape(rows, seq))
        ko_ref[0, i] = k_all.reshape(heads, head_dim, seq)
        vo_ref[0, i] = v_all.reshape(heads, head_dim, seq)
        q_diag = jnp.where(mine, q_s[pl.ds(b, 1), :], 0.0).astype(BF16)
        scores = jnp.dot(q_diag, k_all, preferred_element_type=F32) * scale
        p_s[pl.ds(pl.multiple_of(i * heads, heads), heads), :] = jnp.where(lane <= n, scores, MASK_FILL)
        return carry

    lax.fori_loop(0, per, insert, 0, unroll=UNROLL)
    scores = p_s[...]
    expd = jnp.exp(scores - jnp.max(scores, axis=-1, keepdims=True))
    p_s[...] = (expd / jnp.sum(expd, axis=-1, keepdims=True)).astype(BF16).astype(F32)

    def combine(i, carry):
        probs = p_s[pl.ds(pl.multiple_of(i * heads, heads), heads), :].astype(BF16)
        outs = lax.dot_general(probs, vo_ref[0, i].reshape(rows, seq), (((1,), (1,)), ((), ())),
                               preferred_element_type=F32)
        o_s[pl.ds(i, 1), :] = jnp.sum(jnp.where(mine, outs, 0.0), axis=0, keepdims=True)
        return carry

    lax.fori_loop(0, per, combine, 0, unroll=UNROLL)
    o_ref[...] = o_s[...].astype(BF16)


def attention(layer, part, parts, heads_in, seq_lens, kc, vc, outs):
    _, batch, heads, head_dim, seq = kc.shape
    rows = heads * head_dim
    count = batch // parts
    ready = len(heads_in) == 1
    per = 16
    first = part * count // per
    whole = lambda *shape: pl.BlockSpec(shape, lambda s, n: (0,) * len(shape))
    cache_block = pl.BlockSpec((1, per, heads, head_dim, seq), lambda s, n: (layer, first + s, 0, 0, 0))
    if ready:
        in_specs = [whole(3, rows, seq)]
    else:
        model = heads_in[0].shape[1]
        in_specs = [whole(count, model), whole(1, model), pl.BlockSpec(memory_space=pltpu.HBM),
                    whole(head_dim // 2, seq), whole(head_dim // 2, seq)]
    in_specs += [cache_block, cache_block]
    args = [seq_lens, *heads_in, kc, vc]
    aliases = {}
    if outs is not None:
        in_specs += [pl.BlockSpec(memory_space=pl.ANY)] * 2
        args += list(outs)
        aliases = {len(args) - 2: 1, len(args) - 1: 2}
    if not ready:
        aliases[3] = 3
    w_out = [] if ready else [jax.ShapeDtypeStruct(heads_in[2].shape, BF16)]
    cache_shape = jax.ShapeDtypeStruct(kc.shape, kc.dtype)
    return pl.pallas_call(
        functools.partial(attn_kernel, heads=heads, head_dim=head_dim, scale=head_dim ** -0.5, row0=part * count,
                          ready=ready, layer=layer),
        grid_spec=pltpu.PrefetchScalarGridSpec(
            num_scalar_prefetch=1, grid=(count // per,), in_specs=in_specs,
            out_specs=[pl.BlockSpec((per, rows), lambda s, n: (s, 0)), cache_block, cache_block] + [
                pl.BlockSpec(memory_space=pl.ANY)] * len(w_out),
            scratch_shapes=[pltpu.VMEM((seq, rows), F32), pltpu.VMEM((rows, seq), F32),
                            pltpu.VMEM((rows, seq), F32), pltpu.VMEM((per, rows), F32),
                            pltpu.VMEM((per * heads, seq), F32)] + ([] if ready else [
                                pltpu.VMEM((3 * rows, heads_in[0].shape[1]), BF16), pltpu.SemaphoreType.DMA])),
        out_shape=[jax.ShapeDtypeStruct((count, rows), BF16), cache_shape, cache_shape] + w_out,
        input_output_aliases=aliases,
        compiler_params=pltpu.CompilerParams(dimension_semantics=("arbitrary",), vmem_limit_bytes=28 << 20),
        cost_estimate=pl.CostEstimate(flops=30_000_000_000 // parts, bytes_accessed=kc.size * 4 // parts,
                                      transcendentals=0),
    )(*args)


def solution(mesh):
    cache_spec = P(None, ROW_AXES, None, "tg", None)
    in_specs = (P(ROW_AXES, None), P(ROW_AXES), cache_spec, cache_spec,
                P("pp", None), P("pp", TRAIN_AXES, None), P("pp", None, TRAIN_AXES),
                P("pp", None), P("pp", TRAIN_AXES, None), P("pp", None, TRAIN_AXES))
    out_specs = (P(ROW_AXES, None), cache_spec, cache_spec, P(None, "tg", None), P(None, "tg", None))

    def decode(hidden_in, seq_lens, k_cache, v_cache, attn_gain, w_qkv, w_o, mlp_gain, w_gate_up, w_down):
        layers, batch, _, _, head_dim = k_cache.shape
        model = hidden_in.shape[1]
        stage = lax.axis_index("pp")
        rank = lax.axis_index("tg")
        half = lax.axis_index("grp")
        groups = w_qkv.shape[1] // (3 * head_dim)
        ffn = w_gate_up.shape[1] // 2

        def swap(x, axis):
            return lax.ppermute(x, axis, SWAP)

        def after(x, *deps):
            return lax.optimization_barrier((x,) + deps)[0]

        kc = jnp.transpose(k_cache, (0, 1, 3, 4, 2))
        vc = jnp.transpose(v_cache, (0, 1, 3, 4, 2))

        away_lens = swap(seq_lens, "pp")
        away_in = swap(hidden_in, "pp")
        shard_qkv = w_qkv.reshape(groups, 3, head_dim, model)
        near_qkv = swap(shard_qkv, "grp")
        gains = jnp.stack([attn_gain[0], mlp_gain[0]])
        far_gains = swap(gains, "pp")
        cos_t, sin_t = rope_tables_t(seq_lens, head_dim)
        away_cos, away_sin = rope_tables_t(away_lens, head_dim)
        heads_own, heads_away = project(
            half[None], hidden_in, away_in, attn_gain, shard_qkv, near_qkv,
            jnp.concatenate([cos_t, away_cos], axis=1), jnp.concatenate([sin_t, away_sin], axis=1))
        heads_back = swap(heads_away, "pp")

        shard_o = w_o[0]
        peer_o = swap(shard_o, "tg")
        near_o = swap(shard_o, "grp")
        shard_gu = w_gate_up.reshape(2, ffn, model)
        shard_down = jnp.transpose(w_down[0])
        near_gu = swap(shard_gu, "grp")
        near_down = swap(shard_down, "grp")
        peer_near_o = swap(after(peer_o, heads_own), "grp")

        spots = ((stage, half), (stage, 1 - half), (1 - stage, half), (1 - stage, 1 - half))
        spots = [jnp.stack(spot).astype(jnp.int32) for spot in spots]

        qkv_shape = (layers, 3, 2, groups, head_dim, model)
        gu_shape = (layers, 2, 2, ffn, model)

        def qkv_blocks(pieces, first, many):
            return [(p, (slice(None), t), lambda lay, sh, t=t: (lay, t, sh, pl.ds(first, many)))
                    for p in range(pieces) for t in range(3)]

        def gu_blocks(pieces, lo, hi):
            blocks = []
            for p in range(pieces):
                for t in range(2):
                    a, b = max(lo, t * ffn), min(hi, (t + 1) * ffn)
                    if a < b:
                        blocks.append((p, pl.ds(a - lo, b - a), lambda lay, sh, t=t, a=a, b=b: (
                            lay, t, sh, pl.ds(a - t * ffn, b - a))))
            return blocks

        def qkv_send(i, *deps):
            many = groups // 2
            return swap(after(late_qkv[i * many:(i + 1) * many], *deps), "pp")

        def qkv_take(i, piece, dst):
            many = groups // 2
            near = swap(piece, "grp")
            return place([piece, near], spots[2:], dst, qkv_shape, qkv_blocks(2, i * many, many))

        late_gu = after(w_gate_up[0], heads_own)
        late_qkv = after(shard_qkv, heads_own)
        cuts = [c * ffn // 44 for c in GU_CUTS]

        def gu_send(c, *deps):
            return swap(after((late_gu if c else w_gate_up[0])[cuts[c]:cuts[c + 1]], *deps), "pp")

        def gu_take(c, piece, dst):
            near = swap(piece, "grp")
            return place([piece, near], spots[2:], dst, gu_shape, gu_blocks(2, cuts[c], cuts[c + 1]))

        flat_gu = lambda x: x.reshape(2 * ffn, model)
        gen_qkv = place([shard_qkv, near_qkv], spots[:2], None, qkv_shape, qkv_blocks(2, 0, groups))
        gen_gu = place([flat_gu(shard_gu), flat_gu(near_gu)], spots[:2], None, gu_shape, gu_blocks(2, 0, 2 * ffn))
        sent = [gu_send(0)]
        heads_back = after(heads_back, gen_qkv, gen_gu)
        heads_in = jnp.where(stage == 0, heads_own, heads_back)
        gen_gu = gu_take(0, after(sent[0], heads_own), gen_gu)

        first = jnp.where(stage == 0, gains, far_gains)
        second = jnp.where(stage == 0, far_gains, gains)
        far_heads = [qkv_send(0, heads_back)]
        count = batch // PARTS
        mid = count // 2
        hidden = [hidden_in[i * count:(i + 1) * count] for i in range(PARTS)]
        away = [away_in[i * count:(i + 1) * count] for i in range(PARTS)]
        caches = None
        spot = jnp.stack([rank, half]).astype(jnp.int32)
        for layer, gain in enumerate((first, second)):
            o_vals = []
            for i in range(PARTS):
                if layer == 1 and i == 0:
                    gen_qkv = gen_qkv.reshape(layers, 6 * groups * head_dim, model)
                vals = (heads_in,) if layer == 0 else (hidden[i], gain[0][None], gen_qkv, cos_t, sin_t)
                o_part, *caches = attention(layer, i, PARTS, vals, seq_lens, kc, vc, caches)
                if layer == 1:
                    gen_qkv = caches.pop()
                if layer == 0 and i == 0:
                    far_heads.append(qkv_send(1, o_part))
                if layer == 1 and i == 0:
                    sent.append(gu_send(3, o_part))
                o_vals.append((o_part, swap(o_part, "tg"), swap(o_part, "pp"),
                               lax.ppermute(o_part, ("tg", "pp"), ((0, 3), (1, 2), (2, 1), (3, 0)))))
            last = o_vals[1][0]
            if layer == 0:
                far_heads = [after(x, last) for x in far_heads]
                for i in range(2):
                    gen_qkv = qkv_take(i, far_heads[i], gen_qkv)
                sent.append(gu_send(1, *o_vals[1][1:]))
            else:
                for c in (1, 2, 3):
                    sent[c] = after(sent[c], last)
                    gen_gu = gu_take(c, sent[c], gen_gu)
                sent.append(gu_send(4, *o_vals[1][1:]))
                gen_gu = gu_take(4, sent[4], gen_gu)
            backs, owns = [], []
            give = None
            for i in range(PARTS):
                o_in = tuple(after(x, last) for x in o_vals[i])
                hid = hidden[i]
                if i:
                    hid = after(hid, give)
                keep, give, base = block(spot, o_in, hid, away[i], mlp_gain, (shard_o, near_o, peer_o, peer_near_o),
                                         (shard_gu, near_gu), (shard_down, near_down))
                if i and layer == 0:
                    keep = after(keep, gen_qkv)
                done = (base.astype(F32) + (keep + swap(give, "tg"))).astype(BF16)
                owns.append(done[:mid])
                backs.append(swap(done[mid:], "pp"))
            if layer == 0:
                sent.append(gu_send(2, *backs))
            hidden, away = [], []
            for own, back in zip(owns, backs):
                part = jnp.where(stage == layer, own, back)
                other = swap(part, "tg")
                hidden.append(jnp.concatenate([jnp.where(rank == 0, part, other),
                                               jnp.where(rank == 0, other, part)], axis=0))
                if layer == 0:
                    away.append(swap(hidden[-1], "pp"))
        hidden = jnp.concatenate(hidden, axis=0)

        restore = lambda x: jnp.transpose(x, (0, 1, 4, 2, 3))
        return (hidden, restore(caches[0]), restore(caches[1]), gen_qkv, gen_gu.reshape(layers, 4 * ffn, model))

    return jax.shard_map(decode, mesh=mesh, in_specs=in_specs, out_specs=out_specs, check_vma=False)
```

```python
import functools

import jax
import jax.numpy as jnp
from jax import lax
from jax.experimental import pallas as pl
from jax.experimental.pallas import tpu as pltpu
from jax.sharding import PartitionSpec as P


ROPE_THETA = 500000.0
NORM_EPS = 1e-5
MASK_FILL = -1e30
UNROLL = 16
PARTS = 2
GU_CUTS = (0, 10, 30, 54, 72, 88)
ROW_AXES = ("pp", "grp")
TRAIN_AXES = ("tg", "grp")
SWAP = ((0, 1), (1, 0))
F32 = jnp.float32
BF16 = jnp.bfloat16


def rms_norm(hidden, gain_vec):
    hidden_f32 = hidden.astype(F32)
    inv_rms = lax.rsqrt(jnp.mean(hidden_f32 * hidden_f32, axis=-1, keepdims=True) + NORM_EPS)
    return (hidden_f32 * inv_rms * gain_vec.astype(F32)).astype(BF16)


def rope_tables_t(seq_lens, head_dim):
    inv_freq = jnp.power(ROPE_THETA, -jnp.arange(0, head_dim, 2).astype(F32) / head_dim)
    angles = inv_freq[:, None] * seq_lens.astype(F32)[None, :]
    return jnp.cos(angles), jnp.sin(angles)


def place_kernel(spots_ref, *refs, count, blocks, alias):
    pieces = refs[:count]
    dst = refs[count + alias]
    bufs = refs[count + alias + 1:2 * count + alias + 1]
    sem_in, sem_out = refs[-2:]
    reads, writes = [], []
    for i, (p, src, _) in enumerate(blocks):
        reads.append(pltpu.make_async_copy(pieces[p].at[src], bufs[p].at[src], sem_in.at[i]))
        reads[-1].start()
    for i, (p, src, spot) in enumerate(blocks):
        reads[i].wait()
        target = dst.at[spot(spots_ref[p, 0], spots_ref[p, 1])]
        writes.append(pltpu.make_async_copy(bufs[p].at[src], target, sem_out.at[i]))
        writes[-1].start()
    for write in writes:
        write.wait()


def place(pieces, spots, dst, dst_shape, blocks):
    count, alias = len(pieces), int(dst is not None)
    size = sum(p.size for p in pieces)
    sems = pltpu.SemaphoreType.DMA((len(blocks),))
    return pl.pallas_call(
        functools.partial(place_kernel, count=count, blocks=blocks, alias=alias),
        in_specs=[pl.BlockSpec(memory_space=pltpu.SMEM)] + [pl.BlockSpec(memory_space=pl.ANY)] * (count + alias),
        out_specs=pl.BlockSpec(memory_space=pl.ANY),
        out_shape=jax.ShapeDtypeStruct(dst_shape, BF16),
        scratch_shapes=[pltpu.VMEM(p.shape, BF16) for p in pieces] + [sems, sems],
        input_output_aliases={count + 1: 0} if alias else {},
        compiler_params=pltpu.CompilerParams(vmem_limit_bytes=2 * size + (2 << 20)),
        cost_estimate=pl.CostEstimate(flops=size * 3000, bytes_accessed=size * 4, transcendentals=0),
        name="place",
    )(jnp.stack(spots), *pieces, *([dst] if alias else []))


def rope_t(vals, cos_t, sin_t):
    half = vals.shape[1] // 2
    lo, hi = vals[:, :half], vals[:, half:]
    return jnp.concatenate([lo * cos_t[None] - hi * sin_t[None], hi * cos_t[None] + lo * sin_t[None]], axis=1)


def project_kernel(half_ref, own_ref, away_ref, gain_ref, wa_ref, wb_ref, cos_ref, sin_ref, own_out, away_out):
    groups, _, head_dim, model = wa_ref.shape
    count = own_ref.shape[0]
    rows = groups * head_dim
    normed = rms_norm(jnp.concatenate([own_ref[...], away_ref[...]], axis=0), gain_ref[...])
    for ref, shard in ((wa_ref, half_ref[0]), (wb_ref, 1 - half_ref[0])):
        spot = pl.ds(pl.multiple_of(shard * rows, rows), rows)
        for t in range(3):
            w = ref[:, t].reshape(rows, model)
            vals = lax.dot_general(w, normed, (((1,), (1,)), ((), ())), preferred_element_type=F32)
            if t < 2:
                vals = rope_t(vals.reshape(groups, head_dim, 2 * count), cos_ref[...], sin_ref[...])
                vals = vals.reshape(rows, 2 * count)
            vals = vals.astype(BF16)
            own_out[t, spot, :] = vals[:, :count]
            away_out[t, spot, :] = vals[:, count:]


def project(half, own, away, gain, w_own, w_near, cos_t, sin_t):
    count = own.shape[0]
    out = jax.ShapeDtypeStruct((3, 2 * w_own.shape[0] * w_own.shape[2], count), BF16)
    vmem = pl.BlockSpec(memory_space=pltpu.VMEM)
    return pl.pallas_call(
        project_kernel,
        in_specs=[pl.BlockSpec(memory_space=pltpu.SMEM)] + [vmem] * 7,
        out_specs=[vmem] * 2, out_shape=[out, out],
        compiler_params=pltpu.CompilerParams(vmem_limit_bytes=24 << 20),
        cost_estimate=pl.CostEstimate(flops=3_000_000_000, bytes_accessed=w_own.size * 4, transcendentals=0),
        name="project",
    )(half, own, away, gain, w_own, w_near, cos_t, sin_t)


def block_kernel(place_ref, o_own, o_own_peer, o_away, o_away_peer, hid_ref, away_ref, gain_ref, wo_a, wo_b, wo_c, wo_d,
                 gu_a, gu_b, dn_a, dn_b, keep_ref, give_ref, base_ref, total, rows_s):
    count = hid_ref.shape[0]
    mid = count // 2
    cols = wo_a.shape[1]
    rank, half = place_ref[0], place_ref[1]
    nt = (((1,), (1,)), ((), ()))
    proj = jnp.concatenate([hid_ref[...], away_ref[...]], axis=0).astype(F32)
    out = None
    for (own, away), (near, far) in (((o_own, o_away), (wo_a, wo_b)), ((o_own_peer, o_away_peer), (wo_c, wo_d))):
        o_vals = jnp.concatenate([own[...], away[...]], axis=0).astype(F32)
        lo, hi = o_vals[:, :cols], o_vals[:, cols:]
        mine = jnp.where(half == 0, lo, hi).astype(BF16)
        other = jnp.where(half == 0, hi, lo).astype(BF16)
        for vals, w in ((mine, near), (other, far)):
            part = lax.dot_general(vals, w[...], nt, preferred_element_type=F32)
            out = part if out is None else out + part
    rows = (proj + out).astype(BF16)
    rows_s[...] = rows.astype(F32)
    normed = rms_norm(rows, gain_ref[...])
    for gu, dn in ((gu_a, dn_a), (gu_b, dn_b)):
        gate = lax.dot_general(gu[0], normed, nt, preferred_element_type=F32)
        up = lax.dot_general(gu[1], normed, nt, preferred_element_type=F32)
        act = (jax.nn.silu(gate) * up).T.astype(BF16)
        part = jnp.dot(act, dn[...], preferred_element_type=F32)
        total[...] = part if dn is dn_a else total[...] + part
    mine = pl.multiple_of(rank * mid, mid)
    peer = pl.multiple_of((1 - rank) * mid, mid)
    for i in range(2):
        keep_ref[i * mid:(i + 1) * mid, :] = total[pl.ds(i * count + mine, mid), :]
        give_ref[i * mid:(i + 1) * mid, :] = total[pl.ds(i * count + peer, mid), :]
        base_ref[i * mid:(i + 1) * mid, :] = rows_s[pl.ds(i * count + mine, mid), :].astype(BF16)


def block(spot, o_vals, hid, away, gain, w_o, gus, downs):
    count, model = hid.shape
    ffn = downs[0].shape[0]
    vmem = pl.BlockSpec(memory_space=pltpu.VMEM)
    half_f32 = jax.ShapeDtypeStruct((count, model), F32)
    return pl.pallas_call(
        block_kernel,
        in_specs=[pl.BlockSpec(memory_space=pltpu.SMEM)] + [vmem] * 15,
        out_specs=[vmem] * 3,
        out_shape=[half_f32, half_f32, jax.ShapeDtypeStruct((count, model), BF16)],
        scratch_shapes=[pltpu.VMEM((2 * count, model), F32)] * 2,
        compiler_params=pltpu.CompilerParams(vmem_limit_bytes=32 << 20),
        cost_estimate=pl.CostEstimate(flops=4_000_000_000, bytes_accessed=6 * ffn * model * 2, transcendentals=0),
        name="block",
    )(spot, *o_vals, hid, away, gain, *w_o, *gus, *downs)


def attn_kernel(lens_ref, *rest, heads, head_dim, scale, row0, ready):
    heads_in, rest = rest[:1 if ready else 5], rest[1 if ready else 5:]
    k_ref, v_ref = rest[:2]
    if not ready:
        rest = rest[:-6] + rest[-5:]
    o_ref, ko_ref, vo_ref, q_s, kt_s, vt_s, o_s, p_s = rest[-8:]
    rows = heads * head_dim
    per = k_ref.shape[1]
    seq = k_ref.shape[-1]
    batch = seq
    step = pl.program_id(0)

    @pl.when(step == 0)
    def _():
        if ready:
            for t, ref in enumerate((None, kt_s, vt_s)):
                vals = heads_in[0][t].astype(F32)
                if t:
                    ref[...] = vals
                else:
                    q_s[...] = vals.T
            return
        h_ref, gain_ref, w_ref, cos_ref, sin_ref = heads_in
        normed = rms_norm(h_ref[...], gain_ref[...])
        normed = jnp.concatenate([normed] * (batch // h_ref.shape[0]), axis=0)


        def proj(t, turn):
            vals = lax.dot_general(w_ref[0, t * rows:(t + 1) * rows, :], normed, (((1,), (1,)), ((), ())),
                                   preferred_element_type=F32)
            if turn:
                vals = rope_t(vals.reshape(heads, head_dim, batch), cos_ref[...], sin_ref[...])
            return vals.reshape(rows, batch).astype(BF16).astype(F32)

        q_s[...] = proj(0, True).T
        kt_s[...] = proj(1, True)
        vt_s[...] = proj(2, False)

    lane = lax.broadcasted_iota(jnp.int32, (1, seq), 1)
    head_of = lax.broadcasted_iota(jnp.int32, (heads, rows), 1) // head_dim
    mine = head_of == lax.broadcasted_iota(jnp.int32, (heads, rows), 0)

    def insert(i, carry):
        b = row0 + step * per + i
        n = lens_ref[b]
        shift = lax.rem(n - b + seq, seq)
        at_n = jnp.broadcast_to(lane == n, (rows, seq))
        k_new = pltpu.roll(kt_s[...], shift, 1).astype(BF16)
        v_new = pltpu.roll(vt_s[...], shift, 1).astype(BF16)
        k_all = jnp.where(at_n, k_new, k_ref[0, i].reshape(rows, seq))
        v_all = jnp.where(at_n, v_new, v_ref[0, i].reshape(rows, seq))
        ko_ref[0, i] = k_all.reshape(heads, head_dim, seq)
        vo_ref[0, i] = v_all.reshape(heads, head_dim, seq)
        q_diag = jnp.where(mine, q_s[pl.ds(b, 1), :], 0.0).astype(BF16)
        scores = jnp.dot(q_diag, k_all, preferred_element_type=F32) * scale
        p_s[pl.ds(pl.multiple_of(i * heads, heads), heads), :] = jnp.where(lane <= n, scores, MASK_FILL)
        return carry

    lax.fori_loop(0, per, insert, 0, unroll=UNROLL)
    scores = p_s[...]
    expd = jnp.exp(scores - jnp.max(scores, axis=-1, keepdims=True))
    p_s[...] = (expd / jnp.sum(expd, axis=-1, keepdims=True)).astype(BF16).astype(F32)

    def combine(i, carry):
        probs = p_s[pl.ds(pl.multiple_of(i * heads, heads), heads), :].astype(BF16)
        outs = lax.dot_general(probs, vo_ref[0, i].reshape(rows, seq), (((1,), (1,)), ((), ())),
                               preferred_element_type=F32)
        o_s[pl.ds(i, 1), :] = jnp.sum(jnp.where(mine, outs, 0.0), axis=0, keepdims=True)
        return carry

    lax.fori_loop(0, per, combine, 0, unroll=UNROLL)
    o_ref[...] = o_s[...].astype(BF16)


def attention(layer, part, parts, heads_in, seq_lens, kc, vc, outs):
    _, batch, heads, head_dim, seq = kc.shape
    rows = heads * head_dim
    count = batch // parts
    ready = len(heads_in) == 1
    per = 16
    first = part * count // per
    whole = lambda *shape: pl.BlockSpec(shape, lambda s, n: (0,) * len(shape))
    cache_block = pl.BlockSpec((1, per, heads, head_dim, seq), lambda s, n: (layer, first + s, 0, 0, 0))
    if ready:
        in_specs = [whole(3, rows, seq)]
    else:
        model = heads_in[0].shape[1]
        in_specs = [whole(count, model), whole(1, model), pl.BlockSpec((1, 3 * rows, model), lambda s, n: (layer, 0, 0)),
                    whole(head_dim // 2, seq), whole(head_dim // 2, seq)]
    in_specs += [cache_block, cache_block]
    args = [seq_lens, *heads_in, kc, vc]
    aliases = {}
    if outs is not None:
        in_specs += [pl.BlockSpec(memory_space=pl.ANY)] * 2
        args += list(outs)
        aliases = {len(args) - 2: 1, len(args) - 1: 2}
    if not ready:
        aliases[3] = 3
    w_out = [] if ready else [jax.ShapeDtypeStruct(heads_in[2].shape, BF16)]
    cache_shape = jax.ShapeDtypeStruct(kc.shape, kc.dtype)
    return pl.pallas_call(
        functools.partial(attn_kernel, heads=heads, head_dim=head_dim, scale=head_dim ** -0.5, row0=part * count,
                          ready=ready),
        grid_spec=pltpu.PrefetchScalarGridSpec(
            num_scalar_prefetch=1, grid=(count // per,), in_specs=in_specs,
            out_specs=[pl.BlockSpec((per, rows), lambda s, n: (s, 0)), cache_block, cache_block] + [
                pl.BlockSpec(memory_space=pl.ANY)] * len(w_out),
            scratch_shapes=[pltpu.VMEM((seq, rows), F32), pltpu.VMEM((rows, seq), F32),
                            pltpu.VMEM((rows, seq), F32), pltpu.VMEM((per, rows), F32),
                            pltpu.VMEM((per * heads, seq), F32)]),
        out_shape=[jax.ShapeDtypeStruct((count, rows), BF16), cache_shape, cache_shape] + w_out,
        input_output_aliases=aliases,
        compiler_params=pltpu.CompilerParams(dimension_semantics=("arbitrary",), vmem_limit_bytes=28 << 20),
        cost_estimate=pl.CostEstimate(flops=30_000_000_000 // parts, bytes_accessed=kc.size * 4 // parts,
                                      transcendentals=0),
    )(*args)


def solution(mesh):
    cache_spec = P(None, ROW_AXES, None, "tg", None)
    in_specs = (P(ROW_AXES, None), P(ROW_AXES), cache_spec, cache_spec,
                P("pp", None), P("pp", TRAIN_AXES, None), P("pp", None, TRAIN_AXES),
                P("pp", None), P("pp", TRAIN_AXES, None), P("pp", None, TRAIN_AXES))
    out_specs = (P(ROW_AXES, None), cache_spec, cache_spec, P(None, "tg", None), P(None, "tg", None))

    def decode(hidden_in, seq_lens, k_cache, v_cache, attn_gain, w_qkv, w_o, mlp_gain, w_gate_up, w_down):
        layers, batch, _, _, head_dim = k_cache.shape
        model = hidden_in.shape[1]
        stage = lax.axis_index("pp")
        rank = lax.axis_index("tg")
        half = lax.axis_index("grp")
        groups = w_qkv.shape[1] // (3 * head_dim)
        ffn = w_gate_up.shape[1] // 2

        def swap(x, axis):
            return lax.ppermute(x, axis, SWAP)

        def after(x, *deps):
            return lax.optimization_barrier((x,) + deps)[0]

        kc = jnp.transpose(k_cache, (0, 1, 3, 4, 2))
        vc = jnp.transpose(v_cache, (0, 1, 3, 4, 2))

        away_lens = swap(seq_lens, "pp")
        away_in = swap(hidden_in, "pp")
        shard_qkv = w_qkv.reshape(groups, 3, head_dim, model)
        near_qkv = swap(shard_qkv, "grp")
        gains = jnp.stack([attn_gain[0], mlp_gain[0]])
        far_gains = swap(gains, "pp")
        cos_t, sin_t = rope_tables_t(seq_lens, head_dim)
        away_cos, away_sin = rope_tables_t(away_lens, head_dim)
        heads_own, heads_away = project(
            half[None], hidden_in, away_in, attn_gain, shard_qkv, near_qkv,
            jnp.concatenate([cos_t, away_cos], axis=1), jnp.concatenate([sin_t, away_sin], axis=1))
        heads_back = swap(heads_away, "pp")

        shard_o = w_o[0]
        peer_o = swap(shard_o, "tg")
        near_o = swap(shard_o, "grp")
        shard_gu = w_gate_up.reshape(2, ffn, model)
        shard_down = jnp.transpose(w_down[0])
        near_gu = swap(shard_gu, "grp")
        near_down = swap(shard_down, "grp")
        peer_near_o = swap(after(peer_o, heads_own), "grp")

        spots = ((stage, half), (stage, 1 - half), (1 - stage, half), (1 - stage, 1 - half))
        spots = [jnp.stack(spot).astype(jnp.int32) for spot in spots]

        qkv_shape = (layers, 3, 2, groups, head_dim, model)
        gu_shape = (layers, 2, 2, ffn, model)

        def qkv_blocks(pieces, first, many):
            return [(p, (slice(None), t), lambda lay, sh, t=t: (lay, t, sh, pl.ds(first, many)))
                    for p in range(pieces) for t in range(3)]

        def gu_blocks(pieces, lo, hi):
            blocks = []
            for p in range(pieces):
                for t in range(2):
                    a, b = max(lo, t * ffn), min(hi, (t + 1) * ffn)
                    if a < b:
                        blocks.append((p, pl.ds(a - lo, b - a), lambda lay, sh, t=t, a=a, b=b: (
                            lay, t, sh, pl.ds(a - t * ffn, b - a))))
            return blocks

        def qkv_send(i, *deps):
            many = groups // 2
            return swap(after(late_qkv[i * many:(i + 1) * many], *deps), "pp")

        def qkv_take(i, piece, dst):
            many = groups // 2
            near = swap(piece, "grp")
            return place([piece, near], spots[2:], dst, qkv_shape, qkv_blocks(2, i * many, many))

        late_gu = after(w_gate_up[0], heads_own)
        late_qkv = after(shard_qkv, heads_own)
        cuts = [c * ffn // 44 for c in GU_CUTS]

        def gu_send(c, *deps):
            return swap(after((late_gu if c else w_gate_up[0])[cuts[c]:cuts[c + 1]], *deps), "pp")

        def gu_take(c, piece, dst):
            near = swap(piece, "grp")
            return place([piece, near], spots[2:], dst, gu_shape, gu_blocks(2, cuts[c], cuts[c + 1]))

        flat_gu = lambda x: x.reshape(2 * ffn, model)
        gen_qkv = place([shard_qkv, near_qkv], spots[:2], None, qkv_shape, qkv_blocks(2, 0, groups))
        gen_gu = place([flat_gu(shard_gu), flat_gu(near_gu)], spots[:2], None, gu_shape, gu_blocks(2, 0, 2 * ffn))
        sent = [gu_send(0)]
        heads_back = after(heads_back, gen_qkv, gen_gu)
        heads_in = jnp.where(stage == 0, heads_own, heads_back)
        gen_gu = gu_take(0, after(sent[0], heads_own), gen_gu)

        first = jnp.where(stage == 0, gains, far_gains)
        second = jnp.where(stage == 0, far_gains, gains)
        far_heads = [qkv_send(0, heads_back)]
        count = batch // PARTS
        mid = count // 2
        hidden = [hidden_in[i * count:(i + 1) * count] for i in range(PARTS)]
        away = [away_in[i * count:(i + 1) * count] for i in range(PARTS)]
        caches = None
        spot = jnp.stack([rank, half]).astype(jnp.int32)
        for layer, gain in enumerate((first, second)):
            o_vals = []
            for i in range(PARTS):
                if layer == 1 and i == 0:
                    gen_qkv = gen_qkv.reshape(layers, 6 * groups * head_dim, model)
                vals = (heads_in,) if layer == 0 else (hidden[i], gain[0][None], gen_qkv, cos_t, sin_t)
                o_part, *caches = attention(layer, i, PARTS, vals, seq_lens, kc, vc, caches)
                if layer == 1:
                    gen_qkv = caches.pop()
                if layer == 0 and i == 0:
                    far_heads.append(qkv_send(1, o_part))
                if layer == 1 and i == 0:
                    sent.append(gu_send(3, o_part))
                o_vals.append((o_part, swap(o_part, "tg"), swap(o_part, "pp"),
                               lax.ppermute(o_part, ("tg", "pp"), ((0, 3), (1, 2), (2, 1), (3, 0)))))
            last = o_vals[1][0]
            if layer == 0:
                far_heads = [after(x, last) for x in far_heads]
                for i in range(2):
                    gen_qkv = qkv_take(i, far_heads[i], gen_qkv)
                sent.append(gu_send(1, last))
            else:
                for c in (1, 2, 3):
                    sent[c] = after(sent[c], last)
                    gen_gu = gu_take(c, sent[c], gen_gu)
                sent.append(gu_send(4, last))
                gen_gu = gu_take(4, sent[4], gen_gu)
            backs, owns = [], []
            give = None
            for i in range(PARTS):
                o_in = tuple(after(x, last) for x in o_vals[i])
                hid = hidden[i]
                if i:
                    hid = after(hid, give)
                keep, give, base = block(spot, o_in, hid, away[i], mlp_gain, (shard_o, near_o, peer_o, peer_near_o),
                                         (shard_gu, near_gu), (shard_down, near_down))
                done = (base.astype(F32) + (keep + swap(give, "tg"))).astype(BF16)
                owns.append(done[:mid])
                backs.append(swap(done[mid:], "pp"))
            if layer == 0:
                sent.append(gu_send(2, *backs))
            hidden, away = [], []
            for own, back in zip(owns, backs):
                part = jnp.where(stage == layer, own, back)
                other = swap(part, "tg")
                hidden.append(jnp.concatenate([jnp.where(rank == 0, part, other),
                                               jnp.where(rank == 0, other, part)], axis=0))
                if layer == 0:
                    away.append(swap(hidden[-1], "pp"))
        hidden = jnp.concatenate(hidden, axis=0)

        restore = lambda x: jnp.transpose(x, (0, 1, 4, 2, 3))
        return (hidden, restore(caches[0]), restore(caches[1]), gen_qkv, gen_gu.reshape(layers, 4 * ffn, model))

    return jax.shard_map(decode, mesh=mesh, in_specs=in_specs, out_specs=out_specs, check_vma=False)
```

```python
import functools

import jax
import jax.numpy as jnp
from jax import lax
from jax.experimental import pallas as pl
from jax.experimental.pallas import tpu as pltpu
from jax.sharding import PartitionSpec as P


ROPE_THETA = 500000.0
NORM_EPS = 1e-5
MASK_FILL = -1e30
PER = 8
PARTS = 2
GU_CUTS = (0, 10, 34, 76, 88)
ROW_AXES = ("pp", "grp")
TRAIN_AXES = ("tg", "grp")
SWAP = ((0, 1), (1, 0))
F32 = jnp.float32
BF16 = jnp.bfloat16


def rms_norm(hidden, gain_vec):
    hidden_f32 = hidden.astype(F32)
    inv_rms = lax.rsqrt(jnp.mean(hidden_f32 * hidden_f32, axis=-1, keepdims=True) + NORM_EPS)
    return (hidden_f32 * inv_rms * gain_vec.astype(F32)).astype(BF16)


def rope_tables_t(seq_lens, head_dim):
    inv_freq = jnp.power(ROPE_THETA, -jnp.arange(0, head_dim, 2).astype(F32) / head_dim)
    angles = inv_freq[:, None] * seq_lens.astype(F32)[None, :]
    return jnp.cos(angles), jnp.sin(angles)


def place_kernel(spots_ref, *refs, count, blocks, alias):
    pieces = refs[:count]
    dst = refs[count + alias]
    bufs = refs[count + alias + 1:2 * count + alias + 1]
    sem_in, sem_out = refs[-2:]
    reads, writes = [], []
    for i, (p, src, _) in enumerate(blocks):
        reads.append(pltpu.make_async_copy(pieces[p].at[src], bufs[p].at[src], sem_in.at[i]))
        reads[-1].start()
    for i, (p, src, spot) in enumerate(blocks):
        reads[i].wait()
        target = dst.at[spot(spots_ref[p, 0], spots_ref[p, 1])]
        writes.append(pltpu.make_async_copy(bufs[p].at[src], target, sem_out.at[i]))
        writes[-1].start()
    for write in writes:
        write.wait()


def place(pieces, spots, dst, dst_shape, blocks):
    count, alias = len(pieces), int(dst is not None)
    size = sum(p.size for p in pieces)
    sems = pltpu.SemaphoreType.DMA((len(blocks),))
    return pl.pallas_call(
        functools.partial(place_kernel, count=count, blocks=blocks, alias=alias),
        in_specs=[pl.BlockSpec(memory_space=pltpu.SMEM)] + [pl.BlockSpec(memory_space=pl.ANY)] * (count + alias),
        out_specs=pl.BlockSpec(memory_space=pl.ANY),
        out_shape=jax.ShapeDtypeStruct(dst_shape, BF16),
        scratch_shapes=[pltpu.VMEM(p.shape, BF16) for p in pieces] + [sems, sems],
        input_output_aliases={count + 1: 0} if alias else {},
        compiler_params=pltpu.CompilerParams(vmem_limit_bytes=2 * size + (2 << 20)),
        cost_estimate=pl.CostEstimate(flops=size * 3000, bytes_accessed=size * 4, transcendentals=0),
        name="place",
    )(jnp.stack(spots), *pieces, *([dst] if alias else []))


def rope_t(vals, cos_t, sin_t):
    half = vals.shape[1] // 2
    lo, hi = vals[:, :half], vals[:, half:]
    return jnp.concatenate([lo * cos_t[None] - hi * sin_t[None], hi * cos_t[None] + lo * sin_t[None]], axis=1)


def project_kernel(half_ref, own_ref, away_ref, gain_ref, wa_ref, wb_ref, cos_ref, sin_ref, own_out, away_out):
    groups, _, head_dim, model = wa_ref.shape
    count = own_ref.shape[0]
    rows = groups * head_dim
    normed = rms_norm(jnp.concatenate([own_ref[...], away_ref[...]], axis=0), gain_ref[...])
    for ref, shard in ((wa_ref, half_ref[0]), (wb_ref, 1 - half_ref[0])):
        spot = pl.ds(pl.multiple_of(shard * rows, rows), rows)
        for t in range(3):
            w = ref[:, t].reshape(rows, model)
            vals = lax.dot_general(w, normed, (((1,), (1,)), ((), ())), preferred_element_type=F32)
            if t < 2:
                vals = rope_t(vals.reshape(groups, head_dim, 2 * count), cos_ref[...], sin_ref[...])
                vals = vals.reshape(rows, 2 * count)
            vals = vals.astype(BF16)
            own_out[t, spot, :] = vals[:, :count]
            away_out[t, spot, :] = vals[:, count:]


def project(half, own, away, gain, w_own, w_near, cos_t, sin_t):
    count = own.shape[0]
    out = jax.ShapeDtypeStruct((3, 2 * w_own.shape[0] * w_own.shape[2], count), BF16)
    vmem = pl.BlockSpec(memory_space=pltpu.VMEM)
    return pl.pallas_call(
        project_kernel,
        in_specs=[pl.BlockSpec(memory_space=pltpu.SMEM)] + [vmem] * 7,
        out_specs=[vmem] * 2, out_shape=[out, out],
        compiler_params=pltpu.CompilerParams(vmem_limit_bytes=24 << 20),
        cost_estimate=pl.CostEstimate(flops=3_000_000_000, bytes_accessed=w_own.size * 4, transcendentals=0),
        name="project",
    )(half, own, away, gain, w_own, w_near, cos_t, sin_t)


def block_kernel(place_ref, o_own, o_own_peer, o_away, o_away_peer, hid_ref, away_ref, gain_ref, wo_a, wo_b, wo_c, wo_d,
                 gu_a, gu_b, dn_a, dn_b, keep_ref, give_ref, base_ref, total, rows_s):
    count = hid_ref.shape[0]
    mid = count // 2
    cols = wo_a.shape[1]
    rank, half = place_ref[0], place_ref[1]
    nt = (((1,), (1,)), ((), ()))
    proj = jnp.concatenate([hid_ref[...], away_ref[...]], axis=0).astype(F32)
    out = None
    for (own, away), (near, far) in (((o_own, o_away), (wo_a, wo_b)), ((o_own_peer, o_away_peer), (wo_c, wo_d))):
        o_vals = jnp.concatenate([own[...], away[...]], axis=0).astype(F32)
        lo, hi = o_vals[:, :cols], o_vals[:, cols:]
        mine = jnp.where(half == 0, lo, hi).astype(BF16)
        other = jnp.where(half == 0, hi, lo).astype(BF16)
        for vals, w in ((mine, near), (other, far)):
            part = lax.dot_general(vals, w[...], nt, preferred_element_type=F32)
            out = part if out is None else out + part
    rows = (proj + out).astype(BF16)
    rows_s[...] = rows.astype(F32)
    normed = rms_norm(rows, gain_ref[...])
    for gu, dn in ((gu_a, dn_a), (gu_b, dn_b)):
        gate = lax.dot_general(gu[0], normed, nt, preferred_element_type=F32)
        up = lax.dot_general(gu[1], normed, nt, preferred_element_type=F32)
        act = (jax.nn.silu(gate) * up).T.astype(BF16)
        part = jnp.dot(act, dn[...], preferred_element_type=F32)
        total[...] = part if dn is dn_a else total[...] + part
    mine = pl.multiple_of(rank * mid, mid)
    peer = pl.multiple_of((1 - rank) * mid, mid)
    for i in range(2):
        keep_ref[i * mid:(i + 1) * mid, :] = total[pl.ds(i * count + mine, mid), :]
        give_ref[i * mid:(i + 1) * mid, :] = total[pl.ds(i * count + peer, mid), :]
        base_ref[i * mid:(i + 1) * mid, :] = rows_s[pl.ds(i * count + mine, mid), :].astype(BF16)


def block(spot, o_vals, hid, away, gain, w_o, gus, downs):
    count, model = hid.shape
    ffn = downs[0].shape[0]
    vmem = pl.BlockSpec(memory_space=pltpu.VMEM)
    half_f32 = jax.ShapeDtypeStruct((count, model), F32)
    return pl.pallas_call(
        block_kernel,
        in_specs=[pl.BlockSpec(memory_space=pltpu.SMEM)] + [vmem] * 15,
        out_specs=[vmem] * 3,
        out_shape=[half_f32, half_f32, jax.ShapeDtypeStruct((count, model), BF16)],
        scratch_shapes=[pltpu.VMEM((2 * count, model), F32)] * 2,
        compiler_params=pltpu.CompilerParams(vmem_limit_bytes=32 << 20),
        cost_estimate=pl.CostEstimate(flops=4_000_000_000, bytes_accessed=6 * ffn * model * 2, transcendentals=0),
        name="block",
    )(spot, *o_vals, hid, away, gain, *w_o, *gus, *downs)


def attn_kernel(lens_ref, *rest, heads, head_dim, scale, row0, ready, layer, per):
    heads_in, rest = rest[:1 if ready else 5], rest[1 if ready else 5:]
    k_hbm, v_hbm = rest[:2]
    if not ready:
        w_s, w_sem = rest[-2:]
        rest = rest[:-11] + rest[-10:-2]
    o_ref, ko_hbm, vo_hbm, q_s, kt_s, vt_s, p_s, k_buf, v_buf, sem_in, sem_out = rest[-11:]
    rows = heads * head_dim
    count, seq = k_buf.shape[0], k_buf.shape[-1]
    blocks = count // per

    def moves(blk, out):
        here = pl.ds(blk * per, per)
        there = (layer, pl.ds(row0 + blk * per, per))
        for t, (src, buf, dst) in enumerate(((k_hbm, k_buf, ko_hbm), (v_hbm, v_buf, vo_hbm))):
            if out:
                yield pltpu.make_async_copy(buf.at[here], dst.at[there], sem_out.at[t, blk])
            else:
                yield pltpu.make_async_copy(src.at[there], buf.at[here], sem_in.at[t, blk])

    if not ready:
        fetch = pltpu.make_async_copy(heads_in[2].at[layer], w_s, w_sem)
        fetch.start()
    for blk in range(blocks):
        for move in moves(blk, False):
            move.start()

    if ready:
        q_s[...] = heads_in[0][0].astype(F32).T
        kt_s[...] = heads_in[0][1].astype(F32)
        vt_s[...] = heads_in[0][2].astype(F32)
    else:
        h_ref, gain_ref, _, cos_ref, sin_ref = heads_in
        normed = rms_norm(h_ref[...], gain_ref[...])
        normed = jnp.concatenate([normed] * (seq // count), axis=0)
        fetch.wait()

        def proj(t, turn):
            vals = lax.dot_general(w_s[t * rows:(t + 1) * rows, :], normed, (((1,), (1,)), ((), ())),
                                   preferred_element_type=F32)
            if turn:
                vals = rope_t(vals.reshape(heads, head_dim, seq), cos_ref[...], sin_ref[...])
            return vals.reshape(rows, seq).astype(BF16).astype(F32)

        q_s[...] = proj(0, True).T
        kt_s[...] = proj(1, True)
        vt_s[...] = proj(2, False)

    lane = lax.broadcasted_iota(jnp.int32, (1, seq), 1)
    head_of = lax.broadcasted_iota(jnp.int32, (heads, rows), 1) // head_dim
    mine = head_of == lax.broadcasted_iota(jnp.int32, (heads, rows), 0)

    def one_block(blk, carry):
        for move in moves(blk, False):
            move.wait()
        for i in range(per):
            r = blk * per + i
            b = row0 + r
            n = lens_ref[b]
            shift = lax.rem(n - b + seq, seq)
            at_n = jnp.broadcast_to(lane == n, (rows, seq))
            k_new = pltpu.roll(kt_s[...], shift, 1).astype(BF16)
            v_new = pltpu.roll(vt_s[...], shift, 1).astype(BF16)
            k_all = jnp.where(at_n, k_new, k_buf[r].reshape(rows, seq))
            v_all = jnp.where(at_n, v_new, v_buf[r].reshape(rows, seq))
            k_buf[r] = k_all.reshape(heads, head_dim, seq)
            v_buf[r] = v_all.reshape(heads, head_dim, seq)
            q_diag = jnp.where(mine, q_s[pl.ds(b, 1), :], 0.0).astype(BF16)
            scores = jnp.dot(q_diag, k_all, preferred_element_type=F32) * scale
            p_s[i * heads:(i + 1) * heads, :] = jnp.where(lane <= n, scores, MASK_FILL)
        for move in moves(blk, True):
            move.start()
        scores = p_s[...]
        expd = jnp.exp(scores - jnp.max(scores, axis=-1, keepdims=True))
        probs = (expd / jnp.sum(expd, axis=-1, keepdims=True)).astype(BF16).astype(F32)
        outs = []
        for i in range(per):
            out = lax.dot_general(probs[i * heads:(i + 1) * heads].astype(BF16), v_buf[blk * per + i].reshape(rows, seq),
                                  (((1,), (1,)), ((), ())), preferred_element_type=F32)
            outs.append(jnp.sum(jnp.where(mine, out, 0.0), axis=0, keepdims=True))
        o_ref[pl.ds(pl.multiple_of(blk * per, per), per), :] = jnp.concatenate(outs, axis=0).astype(BF16)
        return carry

    lax.fori_loop(0, blocks, one_block, 0)
    for blk in range(blocks):
        for move in moves(blk, True):
            move.wait()


def attention(layer, part, parts, heads_in, seq_lens, kc, vc, outs):
    _, batch, heads, head_dim, seq = kc.shape
    rows = heads * head_dim
    count = batch // parts
    per = PER
    ready = len(heads_in) == 1
    vmem, hbm = pl.BlockSpec(memory_space=pltpu.VMEM), pl.BlockSpec(memory_space=pl.ANY)
    in_specs = [pl.BlockSpec(memory_space=pltpu.SMEM)] + (
        [vmem] if ready else [vmem, vmem, hbm, vmem, vmem]) + [hbm, hbm]
    args = [seq_lens, *heads_in, kc, vc]
    aliases = {}
    if outs is not None:
        in_specs += [hbm, hbm]
        args += list(outs)
        aliases = {len(args) - 2: 1, len(args) - 1: 2}
    scratch = [pltpu.VMEM((seq, rows), F32), pltpu.VMEM((rows, seq), F32), pltpu.VMEM((rows, seq), F32),
               pltpu.VMEM((per * heads, seq), F32), pltpu.VMEM((count, heads, head_dim, seq), BF16),
               pltpu.VMEM((count, heads, head_dim, seq), BF16),
               pltpu.SemaphoreType.DMA((2, count // per)), pltpu.SemaphoreType.DMA((2, count // per))]
    w_out = []
    if not ready:
        aliases[3] = 3
        w_out = [jax.ShapeDtypeStruct(heads_in[2].shape, BF16)]
        scratch += [pltpu.VMEM(heads_in[2].shape[1:], BF16), pltpu.SemaphoreType.DMA]
    cache_shape = jax.ShapeDtypeStruct(kc.shape, kc.dtype)
    return pl.pallas_call(
        functools.partial(attn_kernel, heads=heads, head_dim=head_dim, scale=head_dim ** -0.5, row0=part * count,
                          ready=ready, layer=layer, per=per),
        in_specs=in_specs, out_specs=[vmem, hbm, hbm] + [hbm] * len(w_out), scratch_shapes=scratch,
        out_shape=[jax.ShapeDtypeStruct((count, rows), BF16), cache_shape, cache_shape] + w_out,
        input_output_aliases=aliases,
        compiler_params=pltpu.CompilerParams(vmem_limit_bytes=28 << 20),
        cost_estimate=pl.CostEstimate(flops=30_000_000_000 // parts, bytes_accessed=kc.size * 4 // parts,
                                      transcendentals=0),
    )(*args)


def solution(mesh):
    cache_spec = P(None, ROW_AXES, None, "tg", None)
    in_specs = (P(ROW_AXES, None), P(ROW_AXES), cache_spec, cache_spec,
                P("pp", None), P("pp", TRAIN_AXES, None), P("pp", None, TRAIN_AXES),
                P("pp", None), P("pp", TRAIN_AXES, None), P("pp", None, TRAIN_AXES))
    out_specs = (P(ROW_AXES, None), cache_spec, cache_spec, P(None, "tg", None), P(None, "tg", None))

    def decode(hidden_in, seq_lens, k_cache, v_cache, attn_gain, w_qkv, w_o, mlp_gain, w_gate_up, w_down):
        layers, batch, _, _, head_dim = k_cache.shape
        model = hidden_in.shape[1]
        stage = lax.axis_index("pp")
        rank = lax.axis_index("tg")
        half = lax.axis_index("grp")
        groups = w_qkv.shape[1] // (3 * head_dim)
        ffn = w_gate_up.shape[1] // 2

        def swap(x, axis):
            return lax.ppermute(x, axis, SWAP)

        def after(x, *deps):
            return lax.optimization_barrier((x,) + deps)[0]

        kc = jnp.transpose(k_cache, (0, 1, 3, 4, 2))
        vc = jnp.transpose(v_cache, (0, 1, 3, 4, 2))

        away_lens = swap(seq_lens, "pp")
        away_in = swap(hidden_in, "pp")
        shard_qkv = w_qkv.reshape(groups, 3, head_dim, model)
        near_qkv = swap(shard_qkv, "grp")
        gains = jnp.stack([attn_gain[0], mlp_gain[0]])
        far_gains = swap(gains, "pp")
        cos_t, sin_t = rope_tables_t(seq_lens, head_dim)
        away_cos, away_sin = rope_tables_t(away_lens, head_dim)
        heads_own, heads_away = project(
            half[None], hidden_in, away_in, attn_gain, shard_qkv, near_qkv,
            jnp.concatenate([cos_t, away_cos], axis=1), jnp.concatenate([sin_t, away_sin], axis=1))
        heads_back = swap(heads_away, "pp")

        shard_o = w_o[0]
        peer_o = swap(shard_o, "tg")
        near_o = swap(shard_o, "grp")
        shard_gu = w_gate_up.reshape(2, ffn, model)
        shard_down = jnp.transpose(w_down[0])
        near_gu = swap(shard_gu, "grp")
        near_down = swap(shard_down, "grp")
        peer_near_o = swap(after(peer_o, heads_own), "grp")

        spots = ((stage, half), (stage, 1 - half), (1 - stage, half), (1 - stage, 1 - half))
        spots = [jnp.stack(spot).astype(jnp.int32) for spot in spots]

        qkv_shape = (layers, 3, 2, groups, head_dim, model)
        gu_shape = (layers, 2, 2, ffn, model)

        def qkv_blocks(pieces, first, many):
            return [(p, (slice(None), t), lambda lay, sh, t=t: (lay, t, sh, pl.ds(first, many)))
                    for p in range(pieces) for t in range(3)]

        def gu_blocks(pieces, lo, hi):
            blocks = []
            for p in range(pieces):
                for t in range(2):
                    a, b = max(lo, t * ffn), min(hi, (t + 1) * ffn)
                    if a < b:
                        blocks.append((p, pl.ds(a - lo, b - a), lambda lay, sh, t=t, a=a, b=b: (
                            lay, t, sh, pl.ds(a - t * ffn, b - a))))
            return blocks

        def qkv_send(i, *deps):
            many = groups // 2
            return swap(after(late_qkv[i * many:(i + 1) * many], *deps), "pp")

        def qkv_take(i, piece, dst):
            many = groups // 2
            near = swap(piece, "grp")
            return place([piece, near], spots[2:], dst, qkv_shape, qkv_blocks(2, i * many, many))

        late_gu = after(w_gate_up[0], heads_own)
        late_qkv = after(shard_qkv, heads_own)
        cuts = [c * ffn // 44 for c in GU_CUTS]

        def gu_send(c, *deps):
            return swap(after((late_gu if c else w_gate_up[0])[cuts[c]:cuts[c + 1]], *deps), "pp")

        def gu_take(c, piece, dst):
            near = swap(piece, "grp")
            return place([piece, near], spots[2:], dst, gu_shape, gu_blocks(2, cuts[c], cuts[c + 1]))

        flat_gu = lambda x: x.reshape(2 * ffn, model)
        gen_qkv = place([shard_qkv, near_qkv], spots[:2], None, qkv_shape, qkv_blocks(2, 0, groups))
        gen_gu = place([flat_gu(shard_gu), flat_gu(near_gu)], spots[:2], None, gu_shape, gu_blocks(2, 0, 2 * ffn))
        sent = [gu_send(0)]
        heads_back = after(heads_back, gen_qkv, gen_gu)
        heads_in = jnp.where(stage == 0, heads_own, heads_back)
        gen_gu = gu_take(0, after(sent[0], heads_own), gen_gu)

        first = jnp.where(stage == 0, gains, far_gains)
        second = jnp.where(stage == 0, far_gains, gains)
        far_heads = [qkv_send(0, heads_back)]
        count = batch // PARTS
        mid = count // 2
        hidden = [hidden_in[i * count:(i + 1) * count] for i in range(PARTS)]
        away = [away_in[i * count:(i + 1) * count] for i in range(PARTS)]
        caches = None
        spot = jnp.stack([rank, half]).astype(jnp.int32)
        for layer, gain in enumerate((first, second)):
            o_vals = []
            for i in range(PARTS):
                if layer == 1 and i == 0:
                    gen_qkv = gen_qkv.reshape(layers, 6 * groups * head_dim, model)
                vals = (heads_in,) if layer == 0 else (hidden[i], gain[0][None], gen_qkv, cos_t, sin_t)
                o_part, *caches = attention(layer, i, PARTS, vals, seq_lens, kc, vc, caches)
                if layer == 1:
                    gen_qkv = caches.pop()
                if layer == 0 and i == 0:
                    far_heads.append(qkv_send(1, o_part))
                o_vals.append((o_part, swap(o_part, "tg"), swap(o_part, "pp"),
                               lax.ppermute(o_part, ("tg", "pp"), ((0, 3), (1, 2), (2, 1), (3, 0)))))
            last = o_vals[1][0]
            if layer == 0:
                far_heads = [after(x, last) for x in far_heads]
                for i in range(2):
                    gen_qkv = qkv_take(i, far_heads[i], gen_qkv)
                sent.append(gu_send(1, last))
            else:
                for c in (1, 2):
                    sent[c] = after(sent[c], last)
                    gen_gu = gu_take(c, sent[c], gen_gu)
                sent.append(gu_send(3, last))
                gen_gu = gu_take(3, sent[3], gen_gu)
            backs, owns = [], []
            give = None
            for i in range(PARTS):
                o_in = tuple(after(x, last) for x in o_vals[i])
                hid = hidden[i]
                if i:
                    hid = after(hid, give)
                keep, give, base = block(spot, o_in, hid, away[i], mlp_gain, (shard_o, near_o, peer_o, peer_near_o),
                                         (shard_gu, near_gu), (shard_down, near_down))
                done = (base.astype(F32) + (keep + swap(give, "tg"))).astype(BF16)
                owns.append(done[:mid])
                backs.append(swap(done[mid:], "pp"))
            if layer == 0:
                sent.append(gu_send(2, *backs))
            hidden, away = [], []
            for own, back in zip(owns, backs):
                part = jnp.where(stage == layer, own, back)
                other = swap(part, "tg")
                hidden.append(jnp.concatenate([jnp.where(rank == 0, part, other),
                                               jnp.where(rank == 0, other, part)], axis=0))
                if layer == 0:
                    away.append(swap(hidden[-1], "pp"))
        hidden = jnp.concatenate(hidden, axis=0)

        restore = lambda x: jnp.transpose(x, (0, 1, 4, 2, 3))
        return (hidden, restore(caches[0]), restore(caches[1]), gen_qkv, gen_gu.reshape(layers, 4 * ffn, model))

    return jax.shard_map(decode, mesh=mesh, in_specs=in_specs, out_specs=out_specs, check_vma=False)
```

```python
import functools

import jax
import jax.numpy as jnp
from jax import lax
from jax.experimental import pallas as pl
from jax.experimental.pallas import tpu as pltpu
from jax.sharding import PartitionSpec as P


ROPE_THETA = 500000.0
NORM_EPS = 1e-5
MASK_FILL = -1e30
PER = 8
PARTS = 2
GU_CUTS = (0, 10, 30, 54, 72, 88)
ROW_AXES = ("pp", "grp")
TRAIN_AXES = ("tg", "grp")
SWAP = ((0, 1), (1, 0))
F32 = jnp.float32
BF16 = jnp.bfloat16


def rms_norm(hidden, gain_vec):
    hidden_f32 = hidden.astype(F32)
    inv_rms = lax.rsqrt(jnp.mean(hidden_f32 * hidden_f32, axis=-1, keepdims=True) + NORM_EPS)
    return (hidden_f32 * inv_rms * gain_vec.astype(F32)).astype(BF16)


def rope_tables_t(seq_lens, head_dim):
    inv_freq = jnp.power(ROPE_THETA, -jnp.arange(0, head_dim, 2).astype(F32) / head_dim)
    angles = inv_freq[:, None] * seq_lens.astype(F32)[None, :]
    return jnp.cos(angles), jnp.sin(angles)


def place_kernel(spots_ref, *refs, count, blocks, alias):
    pieces = refs[:count]
    dst = refs[count + alias]
    bufs = refs[count + alias + 1:2 * count + alias + 1]
    sem_in, sem_out = refs[-2:]
    reads, writes = [], []
    for i, (p, src, _) in enumerate(blocks):
        reads.append(pltpu.make_async_copy(pieces[p].at[src], bufs[p].at[src], sem_in.at[i]))
        reads[-1].start()
    for i, (p, src, spot) in enumerate(blocks):
        reads[i].wait()
        target = dst.at[spot(spots_ref[p, 0], spots_ref[p, 1])]
        writes.append(pltpu.make_async_copy(bufs[p].at[src], target, sem_out.at[i]))
        writes[-1].start()
    for write in writes:
        write.wait()


def place(pieces, spots, dst, dst_shape, blocks):
    count, alias = len(pieces), int(dst is not None)
    size = sum(p.size for p in pieces)
    sems = pltpu.SemaphoreType.DMA((len(blocks),))
    return pl.pallas_call(
        functools.partial(place_kernel, count=count, blocks=blocks, alias=alias),
        in_specs=[pl.BlockSpec(memory_space=pltpu.SMEM)] + [pl.BlockSpec(memory_space=pl.ANY)] * (count + alias),
        out_specs=pl.BlockSpec(memory_space=pl.ANY),
        out_shape=jax.ShapeDtypeStruct(dst_shape, BF16),
        scratch_shapes=[pltpu.VMEM(p.shape, BF16) for p in pieces] + [sems, sems],
        input_output_aliases={count + 1: 0} if alias else {},
        compiler_params=pltpu.CompilerParams(vmem_limit_bytes=2 * size + (2 << 20)),
        cost_estimate=pl.CostEstimate(flops=size * 3000, bytes_accessed=size * 4, transcendentals=0),
        name="place",
    )(jnp.stack(spots), *pieces, *([dst] if alias else []))


def rope_t(vals, cos_t, sin_t):
    half = vals.shape[1] // 2
    lo, hi = vals[:, :half], vals[:, half:]
    return jnp.concatenate([lo * cos_t[None] - hi * sin_t[None], hi * cos_t[None] + lo * sin_t[None]], axis=1)


def project_kernel(half_ref, own_ref, away_ref, gain_ref, wa_ref, wb_ref, cos_ref, sin_ref, own_out, away_out):
    groups, _, head_dim, model = wa_ref.shape
    count = own_ref.shape[0]
    rows = groups * head_dim
    normed = rms_norm(jnp.concatenate([own_ref[...], away_ref[...]], axis=0), gain_ref[...])
    for ref, shard in ((wa_ref, half_ref[0]), (wb_ref, 1 - half_ref[0])):
        spot = pl.ds(pl.multiple_of(shard * rows, rows), rows)
        for t in range(3):
            w = ref[:, t].reshape(rows, model)
            vals = lax.dot_general(w, normed, (((1,), (1,)), ((), ())), preferred_element_type=F32)
            if t < 2:
                vals = rope_t(vals.reshape(groups, head_dim, 2 * count), cos_ref[...], sin_ref[...])
                vals = vals.reshape(rows, 2 * count)
            vals = vals.astype(BF16)
            own_out[t, spot, :] = vals[:, :count]
            away_out[t, spot, :] = vals[:, count:]


def project(half, own, away, gain, w_own, w_near, cos_t, sin_t):
    count = own.shape[0]
    out = jax.ShapeDtypeStruct((3, 2 * w_own.shape[0] * w_own.shape[2], count), BF16)
    vmem = pl.BlockSpec(memory_space=pltpu.VMEM)
    return pl.pallas_call(
        project_kernel,
        in_specs=[pl.BlockSpec(memory_space=pltpu.SMEM)] + [vmem] * 7,
        out_specs=[vmem] * 2, out_shape=[out, out],
        compiler_params=pltpu.CompilerParams(vmem_limit_bytes=24 << 20),
        cost_estimate=pl.CostEstimate(flops=3_000_000_000, bytes_accessed=w_own.size * 4, transcendentals=0),
        name="project",
    )(half, own, away, gain, w_own, w_near, cos_t, sin_t)


def block_kernel(place_ref, o_own, o_own_peer, o_away, o_away_peer, hid_ref, away_ref, gain_ref, wo_a, wo_b, wo_c, wo_d,
                 gu_a, gu_b, dn_a, dn_b, keep_ref, give_ref, base_ref, total, rows_s):
    count = hid_ref.shape[0]
    mid = count // 2
    cols = wo_a.shape[1]
    rank, half = place_ref[0], place_ref[1]
    nt = (((1,), (1,)), ((), ()))
    proj = jnp.concatenate([hid_ref[...], away_ref[...]], axis=0).astype(F32)
    out = None
    for (own, away), (near, far) in (((o_own, o_away), (wo_a, wo_b)), ((o_own_peer, o_away_peer), (wo_c, wo_d))):
        o_vals = jnp.concatenate([own[...], away[...]], axis=0).astype(F32)
        lo, hi = o_vals[:, :cols], o_vals[:, cols:]
        mine = jnp.where(half == 0, lo, hi).astype(BF16)
        other = jnp.where(half == 0, hi, lo).astype(BF16)
        for vals, w in ((mine, near), (other, far)):
            part = lax.dot_general(vals, w[...], nt, preferred_element_type=F32)
            out = part if out is None else out + part
    rows = (proj + out).astype(BF16)
    rows_s[...] = rows.astype(F32)
    normed = rms_norm(rows, gain_ref[...])
    for gu, dn in ((gu_a, dn_a), (gu_b, dn_b)):
        gate = lax.dot_general(gu[0], normed, nt, preferred_element_type=F32)
        up = lax.dot_general(gu[1], normed, nt, preferred_element_type=F32)
        act = (jax.nn.silu(gate) * up).T.astype(BF16)
        part = jnp.dot(act, dn[...], preferred_element_type=F32)
        total[...] = part if dn is dn_a else total[...] + part
    mine = pl.multiple_of(rank * mid, mid)
    peer = pl.multiple_of((1 - rank) * mid, mid)
    for i in range(2):
        keep_ref[i * mid:(i + 1) * mid, :] = total[pl.ds(i * count + mine, mid), :]
        give_ref[i * mid:(i + 1) * mid, :] = total[pl.ds(i * count + peer, mid), :]
        base_ref[i * mid:(i + 1) * mid, :] = rows_s[pl.ds(i * count + mine, mid), :].astype(BF16)


def block(spot, o_vals, hid, away, gain, w_o, gus, downs):
    count, model = hid.shape
    ffn = downs[0].shape[0]
    vmem = pl.BlockSpec(memory_space=pltpu.VMEM)
    half_f32 = jax.ShapeDtypeStruct((count, model), F32)
    return pl.pallas_call(
        block_kernel,
        in_specs=[pl.BlockSpec(memory_space=pltpu.SMEM)] + [vmem] * 15,
        out_specs=[vmem] * 3,
        out_shape=[half_f32, half_f32, jax.ShapeDtypeStruct((count, model), BF16)],
        scratch_shapes=[pltpu.VMEM((2 * count, model), F32)] * 2,
        compiler_params=pltpu.CompilerParams(vmem_limit_bytes=32 << 20),
        cost_estimate=pl.CostEstimate(flops=4_000_000_000, bytes_accessed=6 * ffn * model * 2, transcendentals=0),
        name="block",
    )(spot, *o_vals, hid, away, gain, *w_o, *gus, *downs)


def attn_kernel(lens_ref, *rest, heads, head_dim, scale, row0, ready, layer, per):
    heads_in, rest = rest[:1 if ready else 5], rest[1 if ready else 5:]
    k_hbm, v_hbm = rest[:2]
    if not ready:
        w_s, w_sem = rest[-2:]
        rest = rest[:-11] + rest[-10:-2]
    o_ref, ko_hbm, vo_hbm, q_s, kt_s, vt_s, p_s, k_buf, v_buf, sem_in, sem_out = rest[-11:]
    rows = heads * head_dim
    count, seq = k_buf.shape[0], k_buf.shape[-1]
    blocks = count // per

    def moves(blk, out):
        here = pl.ds(blk * per, per)
        there = (layer, pl.ds(row0 + blk * per, per))
        for t, (src, buf, dst) in enumerate(((k_hbm, k_buf, ko_hbm), (v_hbm, v_buf, vo_hbm))):
            if out:
                yield pltpu.make_async_copy(buf.at[here], dst.at[there], sem_out.at[t, blk])
            else:
                yield pltpu.make_async_copy(src.at[there], buf.at[here], sem_in.at[t, blk])

    if not ready:
        fetch = pltpu.make_async_copy(heads_in[2].at[layer], w_s, w_sem)
        fetch.start()
    head_start = blocks if ready else 2
    for blk in range(head_start):
        for move in moves(blk, False):
            move.start()

    if ready:
        q_s[...] = heads_in[0][0].astype(F32).T
        kt_s[...] = heads_in[0][1].astype(F32)
        vt_s[...] = heads_in[0][2].astype(F32)
    else:
        h_ref, gain_ref, _, cos_ref, sin_ref = heads_in
        normed = rms_norm(h_ref[...], gain_ref[...])
        normed = jnp.concatenate([normed] * (seq // count), axis=0)
        fetch.wait()
        for blk in range(head_start, blocks):
            for move in moves(blk, False):
                move.start()

        def proj(t, turn):
            vals = lax.dot_general(w_s[t * rows:(t + 1) * rows, :], normed, (((1,), (1,)), ((), ())),
                                   preferred_element_type=F32)
            if turn:
                vals = rope_t(vals.reshape(heads, head_dim, seq), cos_ref[...], sin_ref[...])
            return vals.reshape(rows, seq).astype(BF16).astype(F32)

        q_s[...] = proj(0, True).T
        kt_s[...] = proj(1, True)
        vt_s[...] = proj(2, False)

    lane = lax.broadcasted_iota(jnp.int32, (1, seq), 1)
    head_of = lax.broadcasted_iota(jnp.int32, (heads, rows), 1) // head_dim
    mine = head_of == lax.broadcasted_iota(jnp.int32, (heads, rows), 0)

    def one_block(blk, carry):
        for move in moves(blk, False):
            move.wait()
        for i in range(per):
            r = blk * per + i
            b = row0 + r
            n = lens_ref[b]
            shift = lax.rem(n - b + seq, seq)
            at_n = jnp.broadcast_to(lane == n, (rows, seq))
            k_new = pltpu.roll(kt_s[...], shift, 1).astype(BF16)
            v_new = pltpu.roll(vt_s[...], shift, 1).astype(BF16)
            k_all = jnp.where(at_n, k_new, k_buf[r].reshape(rows, seq))
            v_all = jnp.where(at_n, v_new, v_buf[r].reshape(rows, seq))
            k_buf[r] = k_all.reshape(heads, head_dim, seq)
            v_buf[r] = v_all.reshape(heads, head_dim, seq)
            q_diag = jnp.where(mine, q_s[pl.ds(b, 1), :], 0.0).astype(BF16)
            scores = jnp.dot(q_diag, k_all, preferred_element_type=F32) * scale
            p_s[i * heads:(i + 1) * heads, :] = jnp.where(lane <= n, scores, MASK_FILL)
        for move in moves(blk, True):
            move.start()
        scores = p_s[...]
        expd = jnp.exp(scores - jnp.max(scores, axis=-1, keepdims=True))
        probs = (expd / jnp.sum(expd, axis=-1, keepdims=True)).astype(BF16).astype(F32)
        outs = []
        for i in range(per):
            out = lax.dot_general(probs[i * heads:(i + 1) * heads].astype(BF16), v_buf[blk * per + i].reshape(rows, seq),
                                  (((1,), (1,)), ((), ())), preferred_element_type=F32)
            outs.append(jnp.sum(jnp.where(mine, out, 0.0), axis=0, keepdims=True))
        o_ref[pl.ds(pl.multiple_of(blk * per, per), per), :] = jnp.concatenate(outs, axis=0).astype(BF16)
        return carry

    lax.fori_loop(0, blocks, one_block, 0)
    for blk in range(blocks):
        for move in moves(blk, True):
            move.wait()


def attention(layer, part, parts, heads_in, seq_lens, kc, vc, outs):
    _, batch, heads, head_dim, seq = kc.shape
    rows = heads * head_dim
    count = batch // parts
    per = PER
    ready = len(heads_in) == 1
    vmem, hbm = pl.BlockSpec(memory_space=pltpu.VMEM), pl.BlockSpec(memory_space=pl.ANY)
    in_specs = [pl.BlockSpec(memory_space=pltpu.SMEM)] + (
        [vmem] if ready else [vmem, vmem, hbm, vmem, vmem]) + [hbm, hbm]
    args = [seq_lens, *heads_in, kc, vc]
    aliases = {}
    if outs is not None:
        in_specs += [hbm, hbm]
        args += list(outs)
        aliases = {len(args) - 2: 1, len(args) - 1: 2}
    scratch = [pltpu.VMEM((seq, rows), F32), pltpu.VMEM((rows, seq), F32), pltpu.VMEM((rows, seq), F32),
               pltpu.VMEM((per * heads, seq), F32), pltpu.VMEM((count, heads, head_dim, seq), BF16),
               pltpu.VMEM((count, heads, head_dim, seq), BF16),
               pltpu.SemaphoreType.DMA((2, count // per)), pltpu.SemaphoreType.DMA((2, count // per))]
    w_out = []
    if not ready:
        aliases[3] = 3
        w_out = [jax.ShapeDtypeStruct(heads_in[2].shape, BF16)]
        scratch += [pltpu.VMEM(heads_in[2].shape[1:], BF16), pltpu.SemaphoreType.DMA]
    cache_shape = jax.ShapeDtypeStruct(kc.shape, kc.dtype)
    return pl.pallas_call(
        functools.partial(attn_kernel, heads=heads, head_dim=head_dim, scale=head_dim ** -0.5, row0=part * count,
                          ready=ready, layer=layer, per=per),
        in_specs=in_specs, out_specs=[vmem, hbm, hbm] + [hbm] * len(w_out), scratch_shapes=scratch,
        out_shape=[jax.ShapeDtypeStruct((count, rows), BF16), cache_shape, cache_shape] + w_out,
        input_output_aliases=aliases,
        compiler_params=pltpu.CompilerParams(vmem_limit_bytes=28 << 20),
        cost_estimate=pl.CostEstimate(flops=30_000_000_000 // parts, bytes_accessed=kc.size * 4 // parts,
                                      transcendentals=0),
    )(*args)


def solution(mesh):
    cache_spec = P(None, ROW_AXES, None, "tg", None)
    in_specs = (P(ROW_AXES, None), P(ROW_AXES), cache_spec, cache_spec,
                P("pp", None), P("pp", TRAIN_AXES, None), P("pp", None, TRAIN_AXES),
                P("pp", None), P("pp", TRAIN_AXES, None), P("pp", None, TRAIN_AXES))
    out_specs = (P(ROW_AXES, None), cache_spec, cache_spec, P(None, "tg", None), P(None, "tg", None))

    def decode(hidden_in, seq_lens, k_cache, v_cache, attn_gain, w_qkv, w_o, mlp_gain, w_gate_up, w_down):
        layers, batch, _, _, head_dim = k_cache.shape
        model = hidden_in.shape[1]
        stage = lax.axis_index("pp")
        rank = lax.axis_index("tg")
        half = lax.axis_index("grp")
        groups = w_qkv.shape[1] // (3 * head_dim)
        ffn = w_gate_up.shape[1] // 2

        def swap(x, axis):
            return lax.ppermute(x, axis, SWAP)

        def after(x, *deps):
            return lax.optimization_barrier((x,) + deps)[0]

        kc = jnp.transpose(k_cache, (0, 1, 3, 4, 2))
        vc = jnp.transpose(v_cache, (0, 1, 3, 4, 2))

        away_lens = swap(seq_lens, "pp")
        away_in = swap(hidden_in, "pp")
        shard_qkv = w_qkv.reshape(groups, 3, head_dim, model)
        near_qkv = swap(shard_qkv, "grp")
        gains = jnp.stack([attn_gain[0], mlp_gain[0]])
        far_gains = swap(gains, "pp")
        cos_t, sin_t = rope_tables_t(seq_lens, head_dim)
        away_cos, away_sin = rope_tables_t(away_lens, head_dim)
        heads_own, heads_away = project(
            half[None], hidden_in, away_in, attn_gain, shard_qkv, near_qkv,
            jnp.concatenate([cos_t, away_cos], axis=1), jnp.concatenate([sin_t, away_sin], axis=1))
        heads_back = swap(heads_away, "pp")

        shard_o = w_o[0]
        peer_o = swap(shard_o, "tg")
        near_o = swap(shard_o, "grp")
        shard_gu = w_gate_up.reshape(2, ffn, model)
        shard_down = jnp.transpose(w_down[0])
        near_gu = swap(shard_gu, "grp")
        near_down = swap(shard_down, "grp")
        peer_near_o = swap(after(peer_o, heads_own), "grp")

        spots = ((stage, half), (stage, 1 - half), (1 - stage, half), (1 - stage, 1 - half))
        spots = [jnp.stack(spot).astype(jnp.int32) for spot in spots]

        qkv_shape = (layers, 3, 2, groups, head_dim, model)
        gu_shape = (layers, 2, 2, ffn, model)

        def qkv_blocks(pieces, first, many):
            return [(p, (slice(None), t), lambda lay, sh, t=t: (lay, t, sh, pl.ds(first, many)))
                    for p in range(pieces) for t in range(3)]

        def gu_blocks(pieces, lo, hi):
            blocks = []
            for p in range(pieces):
                for t in range(2):
                    a, b = max(lo, t * ffn), min(hi, (t + 1) * ffn)
                    if a < b:
                        blocks.append((p, pl.ds(a - lo, b - a), lambda lay, sh, t=t, a=a, b=b: (
                            lay, t, sh, pl.ds(a - t * ffn, b - a))))
            return blocks

        def qkv_send(i, *deps):
            many = groups // 2
            return swap(after(late_qkv[i * many:(i + 1) * many], *deps), "pp")

        def qkv_take(i, piece, dst):
            many = groups // 2
            near = swap(piece, "grp")
            return place([piece, near], spots[2:], dst, qkv_shape, qkv_blocks(2, i * many, many))

        late_gu = after(w_gate_up[0], heads_own)
        late_qkv = after(shard_qkv, heads_own)
        cuts = [c * ffn // 44 for c in GU_CUTS]

        def gu_send(c, *deps):
            return swap(after((late_gu if c else w_gate_up[0])[cuts[c]:cuts[c + 1]], *deps), "pp")

        def gu_take(c, piece, dst):
            near = swap(piece, "grp")
            return place([piece, near], spots[2:], dst, gu_shape, gu_blocks(2, cuts[c], cuts[c + 1]))

        flat_gu = lambda x: x.reshape(2 * ffn, model)
        gen_qkv = place([shard_qkv, near_qkv], spots[:2], None, qkv_shape, qkv_blocks(2, 0, groups))
        gen_gu = place([flat_gu(shard_gu), flat_gu(near_gu)], spots[:2], None, gu_shape, gu_blocks(2, 0, 2 * ffn))
        sent = [gu_send(0)]
        heads_back = after(heads_back, gen_qkv, gen_gu)
        heads_in = jnp.where(stage == 0, heads_own, heads_back)
        gen_gu = gu_take(0, after(sent[0], heads_own), gen_gu)

        first = jnp.where(stage == 0, gains, far_gains)
        second = jnp.where(stage == 0, far_gains, gains)
        far_heads = [qkv_send(0, heads_back)]
        count = batch // PARTS
        mid = count // 2
        hidden = [hidden_in[i * count:(i + 1) * count] for i in range(PARTS)]
        away = [away_in[i * count:(i + 1) * count] for i in range(PARTS)]
        caches = None
        spot = jnp.stack([rank, half]).astype(jnp.int32)
        for layer, gain in enumerate((first, second)):
            o_vals = []
            for i in range(PARTS):
                if layer == 1 and i == 0:
                    gen_qkv = gen_qkv.reshape(layers, 6 * groups * head_dim, model)
                vals = (heads_in,) if layer == 0 else (hidden[i], gain[0][None], gen_qkv, cos_t, sin_t)
                o_part, *caches = attention(layer, i, PARTS, vals, seq_lens, kc, vc, caches)
                if layer == 1:
                    gen_qkv = caches.pop()
                if layer == 0 and i == 0:
                    far_heads.append(qkv_send(1, o_part))
                if layer == 1 and i == 0:
                    sent.append(gu_send(3, o_part))
                o_vals.append((o_part, swap(o_part, "tg"), swap(o_part, "pp"),
                               lax.ppermute(o_part, ("tg", "pp"), ((0, 3), (1, 2), (2, 1), (3, 0)))))
            last = o_vals[1][0]
            if layer == 0:
                far_heads = [after(x, last) for x in far_heads]
                for i in range(2):
                    gen_qkv = qkv_take(i, far_heads[i], gen_qkv)
                sent.append(gu_send(1, last))
            else:
                for c in (1, 2, 3):
                    sent[c] = after(sent[c], last)
                    gen_gu = gu_take(c, sent[c], gen_gu)
                sent.append(gu_send(4, last))
                gen_gu = gu_take(4, sent[4], gen_gu)
            backs, owns = [], []
            give = None
            for i in range(PARTS):
                o_in = tuple(after(x, last) for x in o_vals[i])
                hid = hidden[i]
                if i:
                    hid = after(hid, give)
                keep, give, base = block(spot, o_in, hid, away[i], mlp_gain, (shard_o, near_o, peer_o, peer_near_o),
                                         (shard_gu, near_gu), (shard_down, near_down))
                done = (base.astype(F32) + (keep + swap(give, "tg"))).astype(BF16)
                owns.append(done[:mid])
                backs.append(swap(done[mid:], "pp"))
            if layer == 0:
                sent.append(gu_send(2, *backs))
            hidden, away = [], []
            for own, back in zip(owns, backs):
                part = jnp.where(stage == layer, own, back)
                other = swap(part, "tg")
                hidden.append(jnp.concatenate([jnp.where(rank == 0, part, other),
                                               jnp.where(rank == 0, other, part)], axis=0))
                if layer == 0:
                    away.append(swap(hidden[-1], "pp"))
        hidden = jnp.concatenate(hidden, axis=0)

        restore = lambda x: jnp.transpose(x, (0, 1, 4, 2, 3))
        return (hidden, restore(caches[0]), restore(caches[1]), gen_qkv, gen_gu.reshape(layers, 4 * ffn, model))

    return jax.shard_map(decode, mesh=mesh, in_specs=in_specs, out_specs=out_specs, check_vma=False)
```
